32 devices in a mesh: groups: 2 (over x), patch: 16 (over z, y, core).
Axes of the slice: x: 2, y: 2, z: 4, core: 2. Of those that a mesh axis runs over, the one named last changes fastest.
Arguments:
- latent: bfloat16 [4, 16, 64, 640], P('groups', 'patch'), parts along dimension 0, may hold values from -6 to 6
- stale_states: bfloat16 [4, 16, 64, 640], P('groups', 'patch'), parts along dimension 0, may hold values from -180 to 180
- stale_sums: float32 [2, 4, 16, 2, 16], P(None, 'groups', 'patch'), parts along dimension 1, as said below
- timestep: int32 [2], P('groups'), parts along dimension 0, may hold values from 0 to 999
- norm_gain: float32 [2, 640], replicated, may hold values from 0.25 to 1.75
- conv_weight: bfloat16 [3, 3, 640, 640], replicated, may hold values from -0.078125 to 0.078125
- time_weight: bfloat16 [320, 640], replicated, may hold values from -0.3125 to 0.3125
- qkv_weight: bfloat16 [3, 640, 640], replicated, may hold values from -0.4375 to 0.4375
- out_weight: bfloat16 [640, 640], replicated, may hold values from -0.25 to 0.25
Outputs:
- block_out: bfloat16 [4, 16, 64, 640], P('groups', 'patch'), parts along dimension 0
- next_states: bfloat16 [4, 16, 64, 640], P('groups', 'patch'), parts along dimension 0
- next_sums: float32 [2, 4, 16, 2, 16], P(None, 'groups', 'patch'), parts along dimension 1
The draws below stay inside these ranges and needn't reach their ends.
There are 2 independent parts, one for each index of `groups`. The reference program is written for one: setup_inputs(seed, part) draws one part's arguments, and reference() takes and returns one part's arrays. A program takes and returns all parts, laid end to end along the dimension named above; an argument that names none is the same for every part. Nothing has to cross between parts.
Inputs may be any that keep to these rules, and one draw needn't show every extreme that they name: `stale_sums`: in every row and group the second entry is at least the square of the first divided by 2560, and more than that.
All inputs are finite; a program needn't handle non-finite values.
Results may differ from the reference program's by a relative error of at most 0.0158.
The reference program's roundings to bfloat16 on the way count: a program that leaves them out, or rounds other values in their place, can miss the bound.
Values may be sent and summed in bfloat16 or wider, within the bound.
A program may use at most 128 MiB of HBM per device.

```python
import math
import jax
import jax.numpy as jnp
from jax import lax

ROWS_DEV = 1
W = 64
C = 640
GROUPS = 16
HEAD_DIM = 64
TFREQ = 320
IMAGES = 2
H = 16


def draw_stale_states(key, part):
    base = jax.random.normal(jax.random.fold_in(key, 11), (IMAGES, H, W, C), jnp.float32)
    base = jnp.clip(base, -6.0, 6.0)
    return base.astype(jnp.bfloat16)


def draw_stale_sums(key, part):
    count = W * (C // GROUPS)
    shape_five = (2, IMAGES, H, 1, GROUPS)
    means = 0.3 * jax.random.normal(jax.random.fold_in(key, 21), shape_five, jnp.float32)
    spread = jnp.exp(jax.random.uniform(jax.random.fold_in(key, 22), shape_five, jnp.float32, -0.7, 0.7))
    position = jnp.arange(H, dtype=jnp.float32) / max(H - 1, 1)
    rising = 1.0 + 2.0 * position
    variances = spread * rising[None, None, :, None, None]
    first = count * means
    second = count * (means * means + variances)
    return jnp.concatenate([first, second], axis=3)


def steps_of(key, dims, pieces, low, largest):
    def one(dim, blocks):
        steps = jax.random.uniform(jax.random.fold_in(jax.random.fold_in(key, 6), dim), (blocks,), jnp.float32, low / len(pieces), largest / len(pieces))
        return jnp.repeat(jnp.exp(steps), dims[dim] // blocks).reshape((-1,) + (1,) * (len(dims) - dim - 1))

    level = one(*pieces[0])
    for cut in pieces[1:]:
        level = level * one(*cut)
    return level


def bell_draw(stream_key, dims, deviation, limit, split=(), kind=jnp.bfloat16):
    values = deviation * jax.random.normal(stream_key, dims, jnp.float32)
    if split:
        values = values * steps_of(stream_key, dims, split, -0.22, 0.18)
    return jnp.clip(values, -limit, limit).astype(kind)


def setup_inputs(seed: int = 0, part: int = 0) -> dict:
    key_of = jax.random.split(jax.random.key(seed), 10)
    part_splits = jax.random.split(jax.random.fold_in(key_of[9], part), 10)
    latent = bell_draw(part_splits[0], (IMAGES, H, W, C), 1.0, 6.0, ((1, 16),))
    stale_states = draw_stale_states(jax.random.fold_in(jax.random.fold_in(key_of[9], part), 71), part)
    stale_sums = draw_stale_sums(jax.random.fold_in(jax.random.fold_in(key_of[9], part), 71), part)
    timestep = jax.random.randint(part_splits[3], (1,), 0, 1000).astype(jnp.int32)
    norm_gain = jnp.clip(1.0 + 0.15 * jax.random.normal(key_of[4], (2, C), jnp.float32), 0.25, 1.75)
    conv_weight = bell_draw(key_of[5], (3, 3, C, C), (9 * C) ** -0.5, 0.078125)
    time_weight = bell_draw(key_of[6], (TFREQ, C), TFREQ ** -0.5, 0.3125)
    qkv_weight = bell_draw(key_of[7], (3, C, C), (C // 3) ** -0.5, 0.4375)
    out_weight = bell_draw(key_of[8], (C, C), C ** -0.5, 0.25)
    return {"latent": latent, "stale_states": stale_states, "stale_sums": stale_sums, "timestep": timestep, "norm_gain": norm_gain, "conv_weight": conv_weight, "time_weight": time_weight, "qkv_weight": qkv_weight, "out_weight": out_weight}


def group_sums(values, groups):
    images, row_count, columns, channels = values.shape
    grouped = values.reshape(images, row_count, columns, groups, channels // groups)
    first = lax.optimization_barrier(jnp.sum(grouped, axis=(2, 4)))
    second = lax.optimization_barrier(jnp.sum(grouped * grouped, axis=(2, 4)))
    return jnp.stack([first, second], axis=2)

def patch_totals(fresh, stale, patches):
    images, height, entries, groups = fresh.shape
    everything = lax.optimization_barrier(jnp.sum(stale, axis=1, keepdims=True))
    own_stale = lax.optimization_barrier(jnp.sum(stale.reshape(images, patches, height // patches, entries, groups), axis=2))
    own_fresh = lax.optimization_barrier(jnp.sum(fresh.reshape(images, patches, height // patches, entries, groups), axis=2))
    per_patch = everything - own_stale + own_fresh
    return jnp.repeat(per_patch, height // patches, axis=1)

def normalize_rows(values, totals, count, gain, groups):
    images, row_count, columns, channels = values.shape
    means = totals[:, :, 0] / count
    spread = totals[:, :, 1] / count - means * means
    inverse = lax.rsqrt(spread + 1e-05)
    grouped = values.reshape(images, row_count, columns, groups, channels // groups)
    scaled = (grouped - means[:, :, None, :, None]) * inverse[:, :, None, :, None]
    return scaled.reshape(values.shape) * gain

def time_embedding(timestep, time_weight):
    half_count = time_weight.shape[0] // 2
    freqs = jnp.exp(-math.log(10000.0) * jnp.arange(half_count, dtype=jnp.float32) / half_count)
    angles = timestep.astype(jnp.float32)[0] * freqs
    embedded = jnp.concatenate([jnp.cos(angles), jnp.sin(angles)])
    return jnp.dot(jax.nn.silu(embedded)[None, :], time_weight.astype(jnp.float32), precision=lax.Precision.HIGHEST)[0]

def project(flat_rows, weight):
    return jnp.dot(flat_rows, weight, preferred_element_type=jnp.float32).astype(jnp.bfloat16)

def reference(latent, stale_states, stale_sums, timestep, norm_gain, conv_weight, time_weight, qkv_weight, out_weight):
    images, height, columns, channels = latent.shape
    heads_count = channels // HEAD_DIM
    count = height * columns * (channels // GROUPS)
    patches = height // ROWS_DEV
    scale = 1.0 / math.sqrt(HEAD_DIM)
    source = latent.astype(jnp.float32)
    fresh_first = group_sums(source, GROUPS)
    totals_first = patch_totals(fresh_first, stale_sums[0], patches)
    active = jax.nn.silu(normalize_rows(source, totals_first, count, norm_gain[0], GROUPS)).astype(jnp.bfloat16)
    padded = jnp.pad(active, ((0, 0), (1, 1), (1, 1), (0, 0)))
    conv = jnp.zeros((images * height * columns, channels), jnp.float32)
    for vertical in range(3):
        for across in range(3):
            window = padded[:, vertical:vertical + height, across:across + columns, :].reshape(-1, channels)
            conv = conv + jnp.dot(window, conv_weight[vertical, across], preferred_element_type=jnp.float32)
    summed = source + conv.reshape(latent.shape) + time_embedding(timestep, time_weight)
    hidden = summed.astype(jnp.bfloat16)
    widened = hidden.astype(jnp.float32)
    fresh_second = group_sums(widened, GROUPS)
    totals_second = patch_totals(fresh_second, stale_sums[1], patches)
    states = normalize_rows(widened, totals_second, count, norm_gain[1], GROUPS).astype(jnp.bfloat16)
    flat_states = states.reshape(-1, channels)
    flat_stale = stale_states.reshape(-1, channels)
    shape_five = (images, height, columns, heads_count, HEAD_DIM)
    queries = project(flat_states, qkv_weight[0]).reshape(images, patches, ROWS_DEV * columns, heads_count, HEAD_DIM)
    fresh_keys = project(flat_states, qkv_weight[1]).reshape(shape_five)
    fresh_values = project(flat_states, qkv_weight[2]).reshape(shape_five)
    stale_keys = project(flat_stale, qkv_weight[1]).reshape(shape_five)
    stale_values = project(flat_stale, qkv_weight[2]).reshape(shape_five)
    row_patch = jnp.arange(height, dtype=jnp.int32) // ROWS_DEV

    def one_patch(index):
        inside = (row_patch == index)[None, :, None, None, None]
        keys_all = jnp.where(inside, fresh_keys, stale_keys).reshape(images, height * columns, heads_count, HEAD_DIM)
        values_all = jnp.where(inside, fresh_values, stale_values).reshape(images, height * columns, heads_count, HEAD_DIM)
        query = lax.dynamic_index_in_dim(queries, index, axis=1, keepdims=False)
        scores = jnp.einsum('bqhd,bkhd->bqhk', query.astype(jnp.float32), keys_all.astype(jnp.float32), precision=lax.Precision.HIGHEST) * scale
        highest = lax.optimization_barrier(jnp.max(scores, axis=3, keepdims=True))
        expo = jnp.exp(scores - highest)
        totals = lax.optimization_barrier(jnp.sum(expo, axis=3))
        weights = expo.astype(jnp.bfloat16)
        mixed = jnp.einsum('bqhk,bkhd->bqhd', weights.astype(jnp.float32), values_all.astype(jnp.float32), precision=lax.Precision.HIGHEST)
        return (mixed / totals[..., None]).astype(jnp.bfloat16)
    results = lax.map(one_patch, jnp.arange(patches, dtype=jnp.int32))
    attended = jnp.moveaxis(results, 0, 1).reshape(-1, channels)
    output = widened + jnp.dot(attended, out_weight, preferred_element_type=jnp.float32).reshape(latent.shape)
    next_sums = jnp.stack([fresh_first, fresh_second], axis=0)
    return (output.astype(jnp.bfloat16), states, next_sums)
```

```python
import functools
import math

import jax
import jax.numpy as jnp
from jax import lax
from jax.experimental import pallas as pl
from jax.experimental.pallas import tpu as pltpu
from jax.sharding import PartitionSpec as P

HEAD_DIM = 64
PACK = 4
EPS = 1e-05


def snake_width(mesh):
    try:
        axis = mesh.axis_names.index("patch")
        line = mesh.devices
        for other in range(line.ndim - 1, -1, -1):
            if other != axis:
                line = line.take(0, axis=other)
        rows = {tuple(d.coords)[1] for d in line.flat}
        return 2 if len(rows) == 2 and tuple(line.flat[2].coords)[1] != tuple(line.flat[0].coords)[1] else 1
    except Exception:
        return 1


def ring_pos(chip, chips, width):
    if width == 1:
        return chip
    long = chips // 2
    z, y = chip // 2, chip % 2
    return z * (1 - y) + (2 * long - 1 - z) * y


def ring_chip(pos, chips, width):
    if width == 1:
        return pos
    long = chips // 2
    y = pos // long
    z = pos * (1 - y) + (2 * long - 1 - pos) * y
    return z * 2 + y


def body(n, width, t_hbm, lat_hbm, stale_hbm, ssum_hbm, gain_hbm, conv_hbm, time_hbm, qkv_hbm, out_hbm,
         block_ref, states_ref, nsums_ref,
         t_ref, lat_ref, stale_ref, gain_ref, conv_w, time_w, qkv_w, out_w, halo, sums_all, sums_out, rx, keys, values,
         act, q_s, att_s, max_s, den_s, mix_s,
         w_sem, small_sem, ring_send, ring_recv, core_send, core_recv, halo_send, halo_recv, sum_send, sum_recv):
    images, _, columns, channels = lat_ref.shape
    groups = ssum_hbm.shape[-1]
    f32, bf16 = jnp.float32, jnp.bfloat16
    tokens = images * columns
    chips, last = n // 2, n // 4
    count = float(n * columns * (channels // groups))
    me = lax.axis_index("patch")
    core = me % 2
    pos = ring_pos(me // 2, chips, width)
    ahead = ring_chip((pos + 1) % chips, chips, width) * 2
    behind = ring_chip((pos + chips - 1) % chips, chips, width) * 2
    target = ahead * (1 - core) + behind * core + core
    sibling = me + 1 - 2 * core
    MESH = pl.DeviceIdType.MESH

    barrier = pltpu.get_barrier_semaphore()

    @pl.loop(1, n)
    def _(d):
        pl.semaphore_signal(barrier, inc=1, device_id={"patch": (me + d) % n}, device_id_type=MESH)

    def load(src, dst, index):
        return pltpu.make_async_copy(src, dst, w_sem.at[index])

    conv_loads = [[load(conv_hbm.at[a, c], conv_w.at[a, c], 3 * a + c) for c in range(3)] for a in range(3)]
    time_load = load(time_hbm, time_w, 9)
    qkv_loads = [load(qkv_hbm.at[i], qkv_w.at[i], 10 + i) for i in range(3)]
    out_load = load(out_hbm, out_w, 13)
    small = [
        pltpu.make_async_copy(src, dst, small_sem.at[i])
        for i, (src, dst) in enumerate(
            ((stale_hbm, stale_ref), (ssum_hbm, sums_all.at[0]), (lat_hbm, lat_ref), (t_hbm, t_ref), (gain_hbm, gain_ref))
        )
    ]
    for copy in small:
        copy.start()
    time_load.start()
    for c in range(3):
        for a in (1, 0, 2):
            conv_loads[a][c].start()
    for i in (0, 1, 2):
        qkv_loads[i].start()
    out_load.start()

    def remote(src, dst, send, recv, where):
        return pltpu.make_async_remote_copy(src_ref=src, dst_ref=dst, send_sem=send, recv_sem=recv,
                                            device_id={"patch": where}, device_id_type=MESH)

    def sum_copy(d):
        return remote(sums_all.at[0], sums_all.at[d], sum_send.at[d], sum_recv.at[d], (me + d) % n)

    def halo_copy(slot):
        where = (me + 1) % n if slot == 0 else (me + n - 1) % n
        return remote(lat_ref, halo.at[slot], halo_send.at[slot], halo_recv.at[slot], where)

    def slot_of(step, direction, row, final):
        return 2 + 4 * (step - 1) + row + (0 if final else 2 * direction)

    def chunk(i, direction):
        return (direction if i < images else 1 - direction), i % images

    def ring_copy(step, i, first=False, final=False):
        row, image = chunk(i, core)
        if first:
            src = stale_ref.at[image, 0] if i < images else rx.at[image, 1]
        else:
            src = rx.at[image, slot_of(step - 1, core, row, False)]
        return remote(src, rx.at[image, slot_of(step, core, row, final)],
                      ring_send.at[step, i], ring_recv.at[step, i], target)

    def core_copy(step, i, final=False, direction=None):
        direction = core if direction is None else direction
        row, image = chunk(i, direction)
        ref = rx.at[image, slot_of(step, direction, row, final)]
        return remote(ref, ref, core_send.at[step, i], core_recv.at[step, i], sibling)

    def own_core_copy(image):
        return remote(stale_ref.at[image, 0], rx.at[image, 1], core_send.at[0, image],
                      core_recv.at[0, image], sibling)

    small[0].wait()
    small[1].wait()
    small[2].wait()
    pl.semaphore_wait(barrier, n - 1)

    for image in range(images):
        own_core_copy(image).start()

    @pl.loop(1, n)
    def _(d):
        sum_copy(d).start()

    for image in range(images):
        ring_copy(1, image, first=True).start()

    @pl.when(me < n - 1)
    def _():
        halo_copy(0).start()

    @pl.when(me > 0)
    def _():
        halo_copy(1).start()

    for image in range(images):
        own_core_copy(image).wait_recv()
        ring_copy(1, images + image, first=True).start()

    def event(step, i, kind):
        ring_copy(step, i, first=True, final=kind == 2).wait_recv()
        if kind == 0 or (kind == 1 and i < images):
            ring_copy(step + 1, i, final=kind == 1).start()
        core_copy(step, i, final=kind == 2).start()

    def count_of(kind):
        return images if kind == 2 else 2 * images

    def kind_of(step):
        return 2 if step == last else 1 if step == last - 1 else 0

    static = [s for s in range(1, last + 1) if last <= 4 or s <= 2]
    queue = [(s, i, kind_of(s)) for s in static for i in range(count_of(kind_of(s)))]

    def pump(amount=1):
        for _ in range(min(amount, len(queue))):
            event(*queue.pop(0))

    def drain(step):
        while queue and queue[0][0] <= step:
            pump()

    def forward(step, kind):
        for i in range(count_of(kind)):
            event(step, i, kind)

    @pl.when(me == 0)
    def _():
        halo[0] = jnp.zeros_like(lat_ref)

    @pl.when(me == n - 1)
    def _():
        halo[1] = jnp.zeros_like(lat_ref)

    def project_rows(image, start, size):
        rows = rx[image, pl.ds(start, size)].reshape(size * columns, channels)
        for which, dest in ((1, keys), (2, values)):
            made = jnp.dot(rows, qkv_w[which], preferred_element_type=f32).astype(bf16)
            dest[image, pl.ds(start, size)] = made.reshape(size, columns, channels)

    def arrived(step, kind):
        for i in range(count_of(kind)):
            core_copy(step, i, final=kind == 2, direction=1 - core).wait_recv()

    def project(step, kind, between=None):
        arrived(step, kind)
        for image in range(images):
            project_rows(image, slot_of(step, 0, 0, kind == 2), 2 if kind == 2 else 4)
            if between is not None:
                between()

    ch = lax.broadcasted_iota(jnp.int32, (channels, groups), 0)
    gr = lax.broadcasted_iota(jnp.int32, (channels, groups), 1) * (channels // groups)
    member = jnp.where((ch >= gr) & (ch < gr + channels // groups), 1.0, 0.0).astype(bf16)
    ch_t = lax.broadcasted_iota(jnp.int32, (groups, channels), 1)
    gr_t = lax.broadcasted_iota(jnp.int32, (groups, channels), 0) * (channels // groups)
    member_t = jnp.where((ch_t >= gr_t) & (ch_t < gr_t + channels // groups), 1.0, 0.0).astype(bf16)

    def exact(x, picks):
        rows = x.shape[0]
        hi = x.astype(bf16)
        rest = x - hi.astype(f32)
        mid = rest.astype(bf16)
        lo = (rest - mid.astype(f32)).astype(bf16)
        y = jnp.dot(jnp.concatenate([hi, mid, lo], axis=0), picks, preferred_element_type=f32)
        return y[2 * rows :] + y[rows : 2 * rows] + y[:rows]

    freq_count = time_w.shape[0] // 2
    idx = lax.broadcasted_iota(jnp.int32, (8, 2 * freq_count), 1)
    low = idx < freq_count
    freqs = jnp.exp(-math.log(10000.0) * jnp.where(low, idx, idx - freq_count).astype(f32) / freq_count)
    small[3].wait()
    small[4].wait()
    angles = t_ref[0].astype(f32) * freqs
    emb = jnp.where(low, jnp.cos(angles), jnp.sin(angles))
    emb = emb / (1.0 + jnp.exp(-emb))
    time_load.wait()
    temb = exact(emb, time_w[...])[0:1]

    pump(2)

    @pl.loop(1, n)
    def _(d):
        sum_copy(d).wait_recv()

    total = sums_all[0]
    total = lax.fori_loop(1, n, lambda d, acc: acc + sums_all[d], total)
    others = [total - sums_all[1], total - sums_all[0], total - sums_all[n - 1]]

    @pl.when(me > 0)
    def _():
        halo_copy(0).wait_recv()

    @pl.when(me < n - 1)
    def _():
        halo_copy(1).wait_recv()

    pump(1)

    def stacked(rows, size):
        pad = size - len(rows)
        if pad:
            rows = rows + [jnp.zeros((pad, rows[0].shape[1]), f32)]
        return jnp.concatenate(rows, axis=0)

    def statistics(blocks, norm, others_of):
        size = -(-len(blocks) // 8) * 8
        firsts = stacked([jnp.sum(x, axis=0, keepdims=True) for x in blocks], size)
        seconds = stacked([jnp.sum(x * x, axis=0, keepdims=True) for x in blocks], size)
        fresh = exact(jnp.concatenate([firsts, seconds], axis=0), member)
        fresh1, fresh2 = fresh[:size], fresh[size:]
        one = stacked([o[norm, b, 0, 0:1] for o, b in others_of], size)
        two = stacked([o[norm, b, 0, 1:2] for o, b in others_of], size)
        m = (one + fresh1) / count
        v = (two + fresh2) / count - m * m
        inv = lax.rsqrt(v + EPS)
        wide = exact(jnp.concatenate([m, inv], axis=0), member_t)
        return fresh1, fresh2, wide[:size], wide[size:]

    def widened(row, image):
        src = lat_ref[image, 0] if row == 1 else halo[0 if row == 0 else 1, image, 0]
        return src.astype(f32)

    pairs = [(r, b) for r in range(3) for b in range(images)]
    fresh1, fresh2, mean, inv = statistics([widened(r, b) for r, b in pairs], 0, [(others[r], b) for r, b in pairs])
    for b in range(images):
        i = images + b
        sums_out[0, b, 0, 0:1] = fresh1[i : i + 1]
        sums_out[0, b, 0, 1:2] = fresh2[i : i + 1]
    pump(1)
    inside = [jnp.where(me > 0, 1.0, 0.0).astype(f32), None, jnp.where(me < n - 1, 1.0, 0.0).astype(f32)]
    for i, (r, b) in enumerate(pairs):
        u = (widened(r, b) - mean[i : i + 1]) * inv[i : i + 1] * gain_ref[0:1, :]
        u = u / (1.0 + jnp.exp(-u))
        if inside[r] is not None:
            u = u * inside[r]
        act[r, pl.ds(b * columns, columns)] = u.astype(bf16)

    def tap(c):
        acc = None
        for a in (1, 0, 2):
            conv_loads[a][c].wait()
            part = jnp.dot(act[a], conv_w[a, c], preferred_element_type=f32)
            acc = part if acc is None else acc + part
        return acc

    place = lax.broadcasted_iota(jnp.int32, (tokens, channels), 0)
    first_col = place == 0
    last_col = place == columns - 1
    for b in range(1, images):
        first_col = first_col | (place == b * columns)
        last_col = last_col | (place == (b + 1) * columns - 1)
    left = jnp.where(first_col, 0.0, pltpu.roll(tap(0), 1, 0))
    pump(1)
    conv = left + tap(1)
    pump(1)
    conv = conv + jnp.where(last_col, 0.0, pltpu.roll(tap(2), tokens - 1, 0))
    lat = jnp.concatenate([widened(1, b) for b in range(images)], axis=0)
    hidden = (lat + conv + temb).astype(bf16)
    wide_hidden = hidden.astype(f32)
    blocks = [wide_hidden[b * columns : (b + 1) * columns] for b in range(images)]
    fresh1, fresh2, mean, inv = statistics(blocks, 1, [(others[1], b) for b in range(images)])
    normed = []
    for b in range(images):
        sums_out[1, b, 0, 0:1] = fresh1[b : b + 1]
        sums_out[1, b, 0, 1:2] = fresh2[b : b + 1]
        s = ((blocks[b] - mean[b : b + 1]) * inv[b : b + 1] * gain_ref[1:2, :]).astype(bf16)
        states_ref[b, 0] = s
        normed.append(s)
    states = jnp.concatenate(normed, axis=0)
    store_sums = pltpu.make_async_copy(sums_out.at[pl.ds(0, 2)], nsums_ref, small_sem.at[5])
    store_sums.start()
    pump(1)

    for load_ in qkv_loads:
        load_.wait()
    q_s[...] = jnp.dot(states, qkv_w[0], preferred_element_type=f32).astype(bf16)
    for which, dest in ((1, keys), (2, values)):
        made = jnp.dot(states, qkv_w[which], preferred_element_type=f32).astype(bf16)
        for b in range(images):
            dest[b, 0] = made[b * columns : (b + 1) * columns]
    pump(1)
    for image in range(images):
        project_rows(image, 1, 1)

    factor = math.log2(math.e) / math.sqrt(HEAD_DIM)

    def attend(start, size, begin, end):
        pack = 0
        for b in range(images):
            for c0 in range(0, channels, PACK * HEAD_DIM):
                c1 = min(c0 + PACK * HEAD_DIM, channels)
                heads = (c1 - c0) // HEAD_DIM
                rows = heads * columns
                qt = q_s[pl.ds(b * columns, columns), c0:c1]
                lane = lax.broadcasted_iota(jnp.int32, (columns, c1 - c0), 1)
                own = [(lane >= h * HEAD_DIM) & (lane < (h + 1) * HEAD_DIM) for h in range(heads)]

                def mixed(x):
                    out = jnp.where(own[0], x[0:columns], 0.0)
                    for h in range(1, heads):
                        out = jnp.where(own[h], x[h * columns : (h + 1) * columns], out)
                    return out

                qb = jnp.concatenate([jnp.where(own[h], qt, jnp.zeros_like(qt)) for h in range(heads)], axis=0)
                kk = keys[b, pl.ds(start, size), :, c0:c1].reshape(size * columns, c1 - c0)
                vv = values[b, pl.ds(start, size), :, c0:c1].reshape(size * columns, c1 - c0)
                s = lax.dot_general(qb, kk, (((1,), (1,)), ((), ())), preferred_element_type=f32)
                top = jnp.max(s, axis=1, keepdims=True)
                if not begin:
                    before = max_s[pack, pl.ds(0, rows)]
                    top = jnp.maximum(top, before)
                e = jnp.exp2((s - top) * factor)
                den = jnp.sum(e, axis=1, keepdims=True)
                mix = mixed(jnp.dot(e.astype(bf16), vv, preferred_element_type=f32))
                if not begin:
                    scale = jnp.exp2((before - top) * factor)
                    den = den + den_s[pack, pl.ds(0, rows)] * scale
                    mix = mix + mix_s[pl.ds(b * columns, columns), c0:c1] * mixed(scale)
                if end:
                    att_s[pl.ds(b * columns, columns), c0:c1] = (mix / mixed(den)).astype(bf16)
                else:
                    max_s[pack, pl.ds(0, rows)] = top
                    den_s[pack, pl.ds(0, rows)] = den
                    mix_s[pl.ds(b * columns, columns), c0:c1] = mix
                pack += 1

    if last <= 4:
        for step in range(1, last - 1):
            drain(step)
            project(step, 0, pump)
        drain(last - 2)
        cut = 2 + 4 * (last - 2)
        attend(0, cut, True, False)
        drain(last - 1)
    else:
        drain(2)
        project(1, 0)

        @pl.loop(3, last - 1)
        def _(step):
            forward(step, 0)
            project(step - 1, 0)

        forward(last - 1, 1)
        project(last - 2, 0)
        cut = 2 + 4 * (last - 2)
        attend(0, cut, True, False)
    project(last - 1, 1)
    if last <= 4:
        drain(last)
    else:
        forward(last, 2)
    project(last, 2)
    attend(cut, n - cut, False, True)

    out_load.wait()
    result = wide_hidden + jnp.dot(att_s[...], out_w[...], preferred_element_type=f32)
    for b in range(images):
        block_ref[b, 0] = result[b * columns : (b + 1) * columns].astype(bf16)

    store_sums.wait()

    @pl.loop(1, n)
    def _(d):
        sum_copy(d).wait_send()

    @pl.when(me < n - 1)
    def _():
        halo_copy(0).wait_send()

    @pl.when(me > 0)
    def _():
        halo_copy(1).wait_send()

    for image in range(images):
        own_core_copy(image).wait_send()
    for i in range(2 * images):
        ring_copy(1, i, first=True).wait_send()

        @pl.loop(2, last)
        def _(step):
            ring_copy(step, i).wait_send()

        @pl.loop(1, last)
        def _(step):
            core_copy(step, i).wait_send()

    for i in range(images):
        ring_copy(last, i, final=True).wait_send()
        core_copy(last, i, final=True).wait_send()


def settle(block_in, states_in, sums_in, block_ref, states_ref, sums_ref, sem):
    copies = [
        pltpu.make_async_copy(src, dst, sem.at[i])
        for i, (src, dst) in enumerate(((block_in, block_ref), (states_in, states_ref), (sums_in, sums_ref)))
    ]
    for copy in copies:
        copy.start()
    for copy in copies:
        copy.wait()


def solution(mesh):
    n = mesh.shape["patch"]
    width = snake_width(mesh)

    def local(latent, stale_states, stale_sums, timestep, norm_gain, conv_weight, time_weight, qkv_weight, out_weight):
        images, row_count, columns, channels = latent.shape
        assert row_count == 1 and n % 4 == 0 and n >= 8 and images % 2 == 0
        vmem = pl.BlockSpec(memory_space=pltpu.VMEM)
        anywhere = pl.BlockSpec(memory_space=pl.ANY)
        bf16 = jnp.bfloat16
        dma = pltpu.SemaphoreType.DMA
        steps = n // 4 + 1
        packs = images * -(-channels // (PACK * HEAD_DIM))
        made = pl.pallas_call(
            functools.partial(body, n, width),
            out_shape=(
                jax.ShapeDtypeStruct(latent.shape, bf16),
                jax.ShapeDtypeStruct(latent.shape, bf16),
                jax.ShapeDtypeStruct(stale_sums.shape, jnp.float32),
            ),
            in_specs=[anywhere] * 9,
            out_specs=(vmem, vmem, anywhere),
            scratch_shapes=[
                pltpu.SMEM(timestep.shape, jnp.int32),
                pltpu.VMEM(latent.shape, bf16),
                pltpu.VMEM(latent.shape, bf16),
                pltpu.VMEM(norm_gain.shape, jnp.float32),
                pltpu.VMEM(conv_weight.shape, bf16),
                pltpu.VMEM(time_weight.shape, bf16),
                pltpu.VMEM(qkv_weight.shape, bf16),
                pltpu.VMEM(out_weight.shape, bf16),
                pltpu.VMEM((2,) + latent.shape, bf16),
                pltpu.VMEM((n + 1,) + stale_sums.shape, jnp.float32),
                pltpu.VMEM((3,) + stale_sums.shape[1:], jnp.float32),
                pltpu.VMEM((images, n, columns, channels), bf16),
                pltpu.VMEM((images, n, columns, channels), bf16),
                pltpu.VMEM((images, n, columns, channels), bf16),
                pltpu.VMEM((3, images * columns, channels), bf16),
                pltpu.VMEM((images * columns, channels), bf16),
                pltpu.VMEM((images * columns, channels), bf16),
                pltpu.VMEM((packs, PACK * columns, 1), jnp.float32),
                pltpu.VMEM((packs, PACK * columns, 1), jnp.float32),
                pltpu.VMEM((images * columns, channels), jnp.float32),
                dma((14,)),
                dma((6,)),
                dma((steps, 2 * images)),
                dma((steps, 2 * images)),
                dma((steps, 2 * images)),
                dma((steps, 2 * images)),
                dma((2,)),
                dma((2,)),
                dma((n,)),
                dma((n,)),
            ],
            compiler_params=pltpu.CompilerParams(
                collective_id=0, has_side_effects=True, vmem_limit_bytes=60 * 1024 * 1024
            ),
        )(timestep, latent, stale_states, stale_sums, norm_gain, conv_weight, time_weight, qkv_weight, out_weight)
        return pl.pallas_call(
            settle,
            out_shape=tuple(jax.ShapeDtypeStruct(x.shape, x.dtype) for x in made),
            in_specs=[vmem] * 3,
            out_specs=(anywhere,) * 3,
            scratch_shapes=[dma((3,))],
        )(*made)

    in_specs = (
        P("groups", "patch", None, None),
        P("groups", "patch", None, None),
        P(None, "groups", "patch", None, None),
        P("groups"),
        P(),
        P(),
        P(),
        P(),
        P(),
    )
    out_specs = (
        P("groups", "patch", None, None),
        P("groups", "patch", None, None),
        P(None, "groups", "patch", None, None),
    )
    return jax.shard_map(local, mesh=mesh, in_specs=in_specs, out_specs=out_specs, check_vma=False)
```

```python
import functools
import math

import jax
import jax.numpy as jnp
from jax import lax
from jax.experimental import pallas as pl
from jax.experimental.pallas import tpu as pltpu
from jax.sharding import PartitionSpec as P

HEAD_DIM = 64
PACK = 4
EPS = 1e-05
PUMPS = (1, 1, 1, 1, 0, 1, 1, 1)


def snake_width(mesh):
    try:
        axis = mesh.axis_names.index("patch")
        line = mesh.devices
        for other in range(line.ndim - 1, -1, -1):
            if other != axis:
                line = line.take(0, axis=other)
        rows = {tuple(d.coords)[1] for d in line.flat}
        return 2 if len(rows) == 2 and tuple(line.flat[2].coords)[1] != tuple(line.flat[0].coords)[1] else 1
    except Exception:
        return 1


def ring_pos(chip, chips, width):
    if width == 1:
        return chip
    long = chips // 2
    z, y = chip // 2, chip % 2
    return z * (1 - y) + (2 * long - 1 - z) * y


def ring_chip(pos, chips, width):
    if width == 1:
        return pos
    long = chips // 2
    y = pos // long
    z = pos * (1 - y) + (2 * long - 1 - pos) * y
    return z * 2 + y


def body(n, width, t_hbm, lat_hbm, stale_hbm, ssum_hbm, gain_hbm, conv_hbm, time_hbm, qkv_hbm, out_hbm,
         block_ref, states_ref, nsums_ref,
         t_ref, lat_ref, stale_ref, gain_ref, conv_w, time_w, qkv_w, out_w, halo, sums_all, sums_out, rx, keys, values,
         act, q_s, flip_w, max_s, den_s, mix_s, block_s, states_s,
         w_sem, small_sem, ring_send, ring_recv, core_send, core_recv, halo_send, halo_recv, sum_send, sum_recv, known):
    images, _, columns, channels = lat_ref.shape
    groups = ssum_hbm.shape[-1]
    f32, bf16 = jnp.float32, jnp.bfloat16
    tokens = images * columns
    chips, last = n // 2, n // 4
    count = float(n * columns * (channels // groups))
    me = lax.axis_index("patch")
    core = me % 2
    pos = ring_pos(me // 2, chips, width)
    ahead = ring_chip((pos + 1) % chips, chips, width) * 2
    behind = ring_chip((pos + chips - 1) % chips, chips, width) * 2
    target = ahead * (1 - core) + behind * core + core
    sibling = me + 1 - 2 * core
    source = ahead * core + behind * (1 - core) + core
    late = me >= n // 2
    MESH = pl.DeviceIdType.MESH

    barrier = pltpu.get_barrier_semaphore()

    def greet(semaphore, where):
        pl.semaphore_signal(semaphore, inc=1, device_id={"patch": where}, device_id_type=MESH)

    greet(barrier, source)
    greet(barrier, sibling)

    def load(src, dst, index):
        return pltpu.make_async_copy(src, dst, w_sem.at[index])

    conv_loads = [
        [load(conv_hbm.at[a, c], conv_w.at[a, :, pl.ds(c * channels, channels)], 3 * a + c) for c in range(3)]
        for a in range(3)
    ]
    time_load = load(time_hbm, time_w, 9)
    qkv_loads = [load(qkv_hbm.at[i], qkv_w.at[i], 10 + i) for i in range(3)]
    out_load = load(out_hbm, out_w, 13)
    small = [
        pltpu.make_async_copy(src, dst, small_sem.at[i])
        for i, (src, dst) in enumerate(
            ((stale_hbm, stale_ref), (ssum_hbm, sums_all.at[0]), (lat_hbm, lat_ref), (t_hbm, t_ref), (gain_hbm, gain_ref))
        )
    ]
    for copy in small:
        copy.start()
    def remote(src, dst, send, recv, where):
        return pltpu.make_async_remote_copy(src_ref=src, dst_ref=dst, send_sem=send, recv_sem=recv,
                                            device_id={"patch": where}, device_id_type=MESH)

    def sum_copy(d):
        return remote(sums_all.at[0], sums_all.at[d], sum_send.at[d], sum_recv.at[d], (me + d) % n)

    def halo_copy(slot):
        where = (me + 1) % n if slot == 0 else (me + n - 1) % n
        return remote(lat_ref, halo.at[slot], halo_send.at[slot], halo_recv.at[slot], where)

    def slot_of(step, direction, row, final):
        return 2 + 4 * (step - 1) + row + (0 if final else 2 * direction)

    def chunk(i, direction):
        return (direction if i < images else 1 - direction), i % images

    def ring_copy(step, i, first=False, final=False):
        row, image = chunk(i, core)
        if first:
            src = stale_ref.at[image, 0] if i < images else rx.at[image, 1]
        else:
            src = rx.at[image, slot_of(step - 1, core, row, False)]
        return remote(src, rx.at[image, slot_of(step, core, row, final)],
                      ring_send.at[step, i], ring_recv.at[step, i], target)

    def core_copy(step, i, final, direction=None):
        direction = core if direction is None else direction
        row, image = chunk(i, direction)
        ref = rx.at[image, slot_of(step, direction, row, final)]
        return remote(ref, ref, core_send.at[step, i], core_recv.at[step, i], sibling)

    def share_copies(step, direction=None):
        direction = core if direction is None else direction
        start = slot_of(step, direction, 0, False)
        begin = pl.multiple_of(start * columns, 2 * columns)
        refs = [keys.at[b, pl.ds(start, 2)] for b in range(images)]
        refs += [values.at[b, :, pl.ds(begin, 2 * columns)] for b in range(images)]
        return [
            remote(ref, ref, core_send.at[step, i], core_recv.at[step, i], sibling) for i, ref in enumerate(refs)
        ]

    def share(step):
        for copy in share_copies(step):
            copy.start()

    def own_core_copy(image):
        return remote(stale_ref.at[image, 0], rx.at[image, 1], core_send.at[0, image],
                      core_recv.at[0, image], sibling)

    for copy in small:
        copy.wait()
    time_load.start()
    qkv_loads[2].start()
    qkv_loads[1].start()
    for a in (1, 0, 2):
        for c in range(3):
            conv_loads[a][c].start()
    qkv_loads[0].start()
    out_load.start()
    pl.semaphore_wait(barrier, 2)

    greet(known.at[0], target)
    for image in range(images):
        own_core_copy(image).start()
    for image in range(images):
        ring_copy(1, image, first=True).start()

    @pl.when(core == 0)
    def _():
        halo_copy(0).start()

    @pl.when(core == 1)
    def _():
        halo_copy(1).start()

    def heard(spread):
        pl.semaphore_wait(known.at[spread], 1)
        if not isinstance(spread, int) or spread < last - 1:
            greet(known.at[spread + 1], target)

    @pl.loop(0, last - 2)
    def _(spread):
        heard(spread)

    for image in range(images):
        own_core_copy(image).wait_recv()
        ring_copy(1, images + image, first=True).start()

    def event(step, i, kind):
        ring_copy(step, i, first=True, final=kind == 2).wait_recv()
        if kind == 0 or (kind == 1 and i < images):
            ring_copy(step + 1, i, final=kind == 1).start()
        if kind:
            core_copy(step, i, kind == 2).start()

    def count_of(kind):
        return images if kind == 2 else 2 * images

    def kind_of(step):
        return 2 if step == last else 1 if step == last - 1 else 0

    static = [s for s in range(1, last + 1) if last <= 4 or s <= 2]
    queue = [(s, i, kind_of(s)) for s in static for i in range(count_of(kind_of(s)))]

    def pump(amount=1):
        for _ in range(min(amount, len(queue))):
            event(*queue.pop(0))

    def drain(step):
        while queue and queue[0][0] <= step:
            pump()

    def forward(step, kind):
        for i in range(count_of(kind)):
            event(step, i, kind)

    @pl.when(me == 0)
    def _():
        halo[0] = jnp.zeros_like(lat_ref)

    @pl.when(me == n - 1)
    def _():
        halo[1] = jnp.zeros_like(lat_ref)

    across = (((1,), (1,)), ((), ()))

    def project_made(pieces):
        rows = jnp.concatenate([piece[2] for piece in pieces], axis=0)
        made = jnp.dot(rows, qkv_w[1], preferred_element_type=f32).astype(bf16)
        turned = lax.dot_general(flip_w[...], rows, across, preferred_element_type=f32).astype(bf16)
        span = 2 * columns
        for i, (image, start, _) in enumerate(pieces):
            at = slice(i * span, (i + 1) * span)
            begin = start * columns
            if not isinstance(begin, int):
                begin = pl.multiple_of(begin, span)
            keys[image, pl.ds(start, 2)] = made[at].reshape(2, columns, channels)
            values[image, :, pl.ds(begin, span)] = turned[:, at]

    def held(image, start):
        return image, start, rx[image, pl.ds(start, 2)].reshape(2 * columns, channels)

    def project(*steps):
        project_made([held(b, slot_of(step, core, 0, False)) for step in steps for b in range(images)])

    def arrived(step):
        for copy in share_copies(step, 1 - core):
            copy.wait_recv()

    def project_raw(step, final):
        for i in range(images if final else 2 * images):
            core_copy(step, i, final, direction=1 - core).wait_recv()
        first = slot_of(step, 0, 0, final)
        starts = [first] if final else [first, first + 2]
        project_made([held(b, start) for b in range(images) for start in starts])

    ch = lax.broadcasted_iota(jnp.int32, (channels, groups), 0)
    gr = lax.broadcasted_iota(jnp.int32, (channels, groups), 1) * (channels // groups)
    member = jnp.where((ch >= gr) & (ch < gr + channels // groups), 1.0, 0.0).astype(bf16)
    ch_t = lax.broadcasted_iota(jnp.int32, (groups, channels), 1)
    gr_t = lax.broadcasted_iota(jnp.int32, (groups, channels), 0) * (channels // groups)
    member_t = jnp.where((ch_t >= gr_t) & (ch_t < gr_t + channels // groups), 1.0, 0.0).astype(bf16)

    def exact(x, picks):
        rows = x.shape[0]
        hi = x.astype(bf16)
        rest = x - hi.astype(f32)
        mid = rest.astype(bf16)
        lo = (rest - mid.astype(f32)).astype(bf16)
        y = jnp.dot(jnp.concatenate([hi, mid, lo], axis=0), picks, preferred_element_type=f32)
        return y[2 * rows :] + y[rows : 2 * rows] + y[:rows]

    firsts = [queue.pop(0) for _ in range(3)]

    @pl.when(jnp.logical_not(late))
    def _():
        event(*firsts[0])

    heard(last - 2)

    @pl.when(jnp.logical_not(late))
    def _():
        event(*firsts[1])
        event(*firsts[2])

    heard(last - 1)
    greet(known.at[last], sibling)
    pl.semaphore_wait(known.at[last], 1)

    @pl.loop(1, n)
    def _(d):
        sum_copy(d).start()

    @pl.when((core == 1) & (me < n - 1))
    def _():
        halo_copy(0).start()

    @pl.when((core == 0) & (me > 0))
    def _():
        halo_copy(1).start()

    @pl.when(late)
    def _():
        for first in firsts:
            event(*first)

    freq_count = time_w.shape[0] // 2
    idx = lax.broadcasted_iota(jnp.int32, (8, 2 * freq_count), 1)
    low = idx < freq_count
    freqs = jnp.exp(-math.log(10000.0) * jnp.where(low, idx, idx - freq_count).astype(f32) / freq_count)
    angles = t_ref[...].astype(f32) * freqs
    emb = jnp.where(low, jnp.cos(angles), jnp.sin(angles))
    emb = emb / (1.0 + jnp.exp(-emb))
    time_load.wait()
    temb = exact(emb, time_w[...])[0:1]

    qkv_loads[2].wait()
    diagonal = lax.broadcasted_iota(jnp.int32, (channels, channels), 0) == lax.broadcasted_iota(
        jnp.int32, (channels, channels), 1
    )
    unit = jnp.where(diagonal, 1.0, 0.0).astype(bf16)
    flip_w[...] = lax.dot_general(unit, qkv_w[2], across, preferred_element_type=f32).astype(bf16)

    drain(1)
    qkv_loads[1].wait()
    project(1)
    pump(PUMPS[0])
    share(1)

    @pl.loop(1, n)
    def _(d):
        sum_copy(d).wait_recv()

    total = sums_all[0]
    total = lax.fori_loop(1, n, lambda d, acc: acc + sums_all[d], total)
    others = [total - sums_all[1], total - sums_all[0], total - sums_all[n - 1]]

    @pl.when(me > 0)
    def _():
        halo_copy(0).wait_recv()

    @pl.when(me < n - 1)
    def _():
        halo_copy(1).wait_recv()

    pump(PUMPS[1])

    def stacked(rows, size):
        pad = size - len(rows)
        if pad:
            rows = rows + [jnp.zeros((pad, rows[0].shape[1]), f32)]
        return jnp.concatenate(rows, axis=0)

    def statistics(blocks, norm, others_of):
        size = -(-len(blocks) // 8) * 8
        firsts = stacked([jnp.sum(x, axis=0, keepdims=True) for x in blocks], size)
        seconds = stacked([jnp.sum(x * x, axis=0, keepdims=True) for x in blocks], size)
        fresh = exact(jnp.concatenate([firsts, seconds], axis=0), member)
        fresh1, fresh2 = fresh[:size], fresh[size:]
        one = stacked([o[norm, b, 0, 0:1] for o, b in others_of], size)
        two = stacked([o[norm, b, 0, 1:2] for o, b in others_of], size)
        m = (one + fresh1) / count
        v = (two + fresh2) / count - m * m
        inv = lax.rsqrt(v + EPS)
        wide = exact(jnp.concatenate([m, inv], axis=0), member_t)
        return fresh1, fresh2, wide[:size], wide[size:]

    def widened(row, image):
        src = lat_ref[image, 0] if row == 1 else halo[0 if row == 0 else 1, image, 0]
        return src.astype(f32)

    pairs = [(r, b) for r in range(3) for b in range(images)]
    fresh1, fresh2, mean, inv = statistics([widened(r, b) for r, b in pairs], 0, [(others[r], b) for r, b in pairs])
    for b in range(images):
        i = images + b
        sums_out[0, b, 0, 0:1] = fresh1[i : i + 1]
        sums_out[0, b, 0, 1:2] = fresh2[i : i + 1]
    pump(PUMPS[2])
    inside = [jnp.where(me > 0, 1.0, 0.0).astype(f32), None, jnp.where(me < n - 1, 1.0, 0.0).astype(f32)]
    for i, (r, b) in enumerate(pairs):
        u = (widened(r, b) - mean[i : i + 1]) * inv[i : i + 1] * gain_ref[0:1, :]
        u = u / (1.0 + jnp.exp(-u))
        if inside[r] is not None:
            u = u * inside[r]
        act[r, pl.ds(b * columns, columns)] = u.astype(bf16)

    taps = None
    for a in (1, 0, 2):
        for c in range(3):
            conv_loads[a][c].wait()
        part = jnp.dot(act[a], conv_w[a], preferred_element_type=f32)
        taps = part if taps is None else taps + part
    taps = [taps[:, c * channels : (c + 1) * channels] for c in range(3)]

    place = lax.broadcasted_iota(jnp.int32, (tokens, channels), 0)
    first_col = place == 0
    last_col = place == columns - 1
    for b in range(1, images):
        first_col = first_col | (place == b * columns)
        last_col = last_col | (place == (b + 1) * columns - 1)
    conv = jnp.where(first_col, 0.0, pltpu.roll(taps[0], 1, 0)) + taps[1]
    conv = conv + jnp.where(last_col, 0.0, pltpu.roll(taps[2], tokens - 1, 0))
    pump(PUMPS[3])
    if last <= 4:
        for step in range(2, last - 1):
            drain(step)
            project(step)
            share(step)
    lat = jnp.concatenate([widened(1, b) for b in range(images)], axis=0)
    hidden = (lat + conv + temb).astype(bf16)
    wide_hidden = hidden.astype(f32)
    blocks = [wide_hidden[b * columns : (b + 1) * columns] for b in range(images)]
    fresh1, fresh2, mean, inv = statistics(blocks, 1, [(others[1], b) for b in range(images)])
    normed = []
    for b in range(images):
        sums_out[1, b, 0, 0:1] = fresh1[b : b + 1]
        sums_out[1, b, 0, 1:2] = fresh2[b : b + 1]
        s = ((blocks[b] - mean[b : b + 1]) * inv[b : b + 1] * gain_ref[1:2, :]).astype(bf16)
        states_s[b, 0] = s
        normed.append(s)
    states = jnp.concatenate(normed, axis=0)
    store_sums = pltpu.make_async_copy(sums_out.at[pl.ds(0, 2)], nsums_ref, small_sem.at[5])
    store_sums.start()
    store_states = pltpu.make_async_copy(states_s, states_ref, small_sem.at[6])
    store_states.start()
    pump(PUMPS[5])

    qkv_loads[0].wait()
    q_s[...] = jnp.dot(states, qkv_w[0], preferred_element_type=f32).astype(bf16)
    project_made([(b, 0, jnp.concatenate([normed[b], rx[b, 1]], axis=0)) for b in range(images)])
    pump(PUMPS[6])

    factor = math.log2(math.e) / math.sqrt(HEAD_DIM)

    pair = 2 * columns

    def sent():
        store_sums.wait()
        store_states.wait()

        @pl.loop(1, n)
        def _(d):
            sum_copy(d).wait_send()

        @pl.when(me < n - 1)
        def _():
            halo_copy(0).wait_send()

        @pl.when(me > 0)
        def _():
            halo_copy(1).wait_send()

        for image in range(images):
            own_core_copy(image).wait_send()
        for i in range(2 * images):
            ring_copy(1, i, first=True).wait_send()

            @pl.loop(2, last)
            def _(step):
                ring_copy(step, i).wait_send()

        @pl.loop(1, last - 1)
        def _(step):
            for copy in share_copies(step):
                copy.wait_send()

    def attend(start, size, begin, end):
        spans = [
            (b, c0, min(c0 + PACK * HEAD_DIM, channels))
            for b in range(images)
            for c0 in range(0, channels, PACK * HEAD_DIM)
        ]

        def score(b, c0, c1):
            heads = (c1 - c0) // HEAD_DIM
            qt = q_s[pl.ds(b * columns, columns), c0:c1]
            lane = lax.broadcasted_iota(jnp.int32, (columns, c1 - c0), 1)
            own = [(lane >= h * HEAD_DIM) & (lane < (h + 1) * HEAD_DIM) for h in range(heads)]
            qb = jnp.concatenate([jnp.where(own[h], qt, jnp.zeros_like(qt)) for h in range(heads)], axis=0)
            kk = keys[b, pl.ds(start, size), :, c0:c1].reshape(size * columns, c1 - c0)
            return lax.dot_general(kk, qb, across, preferred_element_type=f32)

        blocks_of = [[] for _ in range(images)]
        ahead_s = score(*spans[0])
        for pack, (b, c0, c1) in enumerate(spans):
            heads = (c1 - c0) // HEAD_DIM
            rows = heads * columns
            s = ahead_s
            if pack + 1 < len(spans):
                ahead_s = score(*spans[pack + 1])
            vv = values[b, c0:c1, pl.ds(start * columns, size * columns)]
            top = jnp.max(s, axis=0, keepdims=True)
            if not begin:
                before = max_s[pack, :, pl.ds(0, rows)]
                top = jnp.maximum(top, before)
            e = jnp.exp2((s - top) * factor)
            den = jnp.sum(e, axis=0, keepdims=True)
            if not begin:
                scale = jnp.exp2((before - top) * factor)
                den = den + den_s[pack, :, pl.ds(0, rows)] * scale
            o = jnp.dot(vv, e.astype(bf16), preferred_element_type=f32)
            if not end:
                max_s[pack, :, pl.ds(0, rows)] = top
                den_s[pack, :, pl.ds(0, rows)] = den
            for h in range(heads):
                j = h // 2 * pair
                at = pl.ds(c0 + h * HEAD_DIM, HEAD_DIM)
                part = o[h * HEAD_DIM : (h + 1) * HEAD_DIM, j : j + pair]
                if not begin:
                    part = part + mix_s[b, at] * scale[:, j : j + pair]
                if not end:
                    mix_s[b, at] = part
                else:
                    part = part / den[:, j : j + pair]
                    blocks_of[b].append(part if h % 2 == b % 2 else pltpu.roll(part, columns, 1))
        if end:
            lane = lax.broadcasted_iota(jnp.int32, (HEAD_DIM, pair), 1)
            merged = [jnp.where(lane < columns, x, y) for x, y in zip(*blocks_of)]
            return jnp.concatenate(merged, axis=0).astype(bf16)

    if last > 4:
        drain(2)

        @pl.loop(3, last - 1)
        def _(step):
            forward(step, 0)
            project(step - 1)
            share(step - 1)

        project(last - 2)
        share(last - 2)

    @pl.loop(1, last - 1)
    def _(step):
        arrived(step)

    cut = slot_of(last - 1, 0, 0, False)
    if last <= 4:
        pump(PUMPS[7])
    attend(0, cut, True, False)
    sent()
    if last <= 4:
        drain(last - 1)
    else:
        forward(last - 1, 1)
    project_raw(last - 1, False)
    if last <= 4:
        drain(last)
    else:
        forward(last, 2)
    project_raw(last, True)
    attended = attend(cut, n - cut, False, True)

    out_load.wait()
    result = wide_hidden + lax.dot_general(
        attended, out_w[...], (((0,), (0,)), ((), ())), preferred_element_type=f32
    )
    for b in range(images):
        block_s[b, 0] = result[b * columns : (b + 1) * columns].astype(bf16)
    store_block = pltpu.make_async_copy(block_s, block_ref, small_sem.at[7])
    store_block.start()
    for i in range(2 * images):
        core_copy(last - 1, i, False).wait_send()
    for i in range(images):
        ring_copy(last, i, final=True).wait_send()
        core_copy(last, i, True).wait_send()
    store_block.wait()


def settle(block_in, states_in, sums_in, block_ref, states_ref, sums_ref, sem):
    copies = [
        pltpu.make_async_copy(src, dst, sem.at[i])
        for i, (src, dst) in enumerate(((block_in, block_ref), (states_in, states_ref), (sums_in, sums_ref)))
    ]
    for copy in copies:
        copy.start()
    for copy in copies:
        copy.wait()


def solution(mesh):
    n = mesh.shape["patch"]
    width = snake_width(mesh)

    def local(latent, stale_states, stale_sums, timestep, norm_gain, conv_weight, time_weight, qkv_weight, out_weight):
        images, row_count, columns, channels = latent.shape
        assert row_count == 1 and n % 4 == 0 and n >= 8 and images == 2 and columns == HEAD_DIM
        vmem = pl.BlockSpec(memory_space=pltpu.VMEM)
        anywhere = pl.BlockSpec(memory_space=pl.ANY)
        bf16 = jnp.bfloat16
        dma = pltpu.SemaphoreType.DMA
        steps = n // 4 + 1
        packs = images * -(-channels // (PACK * HEAD_DIM))
        made = pl.pallas_call(
            functools.partial(body, n, width),
            out_shape=(
                jax.ShapeDtypeStruct(latent.shape, bf16),
                jax.ShapeDtypeStruct(latent.shape, bf16),
                jax.ShapeDtypeStruct(stale_sums.shape, jnp.float32),
            ),
            in_specs=[pl.BlockSpec(memory_space=pltpu.HBM)] * 9,
            out_specs=(pl.BlockSpec(memory_space=pltpu.HBM),) * 3,
            scratch_shapes=[
                pltpu.VMEM((1, 1), jnp.int32),
                pltpu.VMEM(latent.shape, bf16),
                pltpu.VMEM(latent.shape, bf16),
                pltpu.VMEM(norm_gain.shape, jnp.float32),
                pltpu.VMEM((3, channels, 3 * channels), bf16),
                pltpu.VMEM(time_weight.shape, bf16),
                pltpu.VMEM(qkv_weight.shape, bf16),
                pltpu.VMEM(out_weight.shape, bf16),
                pltpu.VMEM((2,) + latent.shape, bf16),
                pltpu.VMEM((n + 1,) + stale_sums.shape, jnp.float32),
                pltpu.VMEM((3,) + stale_sums.shape[1:], jnp.float32),
                pltpu.VMEM((images, n, columns, channels), bf16),
                pltpu.VMEM((images, n, columns, channels), bf16),
                pltpu.VMEM((images, channels, n * columns), bf16),
                pltpu.VMEM((3, images * columns, channels), bf16),
                pltpu.VMEM((images * columns, channels), bf16),
                pltpu.VMEM((channels, channels), bf16),
                pltpu.VMEM((packs, 1, PACK * columns), jnp.float32),
                pltpu.VMEM((packs, 1, PACK * columns), jnp.float32),
                pltpu.VMEM((images, channels, 2 * columns), jnp.float32),
                pltpu.VMEM(latent.shape, bf16),
                pltpu.VMEM(latent.shape, bf16),
                dma((14,)),
                dma((8,)),
                dma((steps, 2 * images)),
                dma((steps, 2 * images)),
                dma((steps, 2 * images)),
                dma((steps, 2 * images)),
                dma((2,)),
                dma((2,)),
                dma((n,)),
                dma((n,)),
                pltpu.SemaphoreType.REGULAR((n // 4 + 1,)),
            ],
            compiler_params=pltpu.CompilerParams(
                collective_id=0, has_side_effects=True, vmem_limit_bytes=60 * 1024 * 1024
            ),
        )(timestep.reshape(1, 1), latent, stale_states, stale_sums, norm_gain, conv_weight, time_weight, qkv_weight, out_weight)
        return pl.pallas_call(
            settle,
            out_shape=tuple(jax.ShapeDtypeStruct(x.shape, x.dtype) for x in made),
            in_specs=[vmem] * 3,
            out_specs=(anywhere,) * 3,
            scratch_shapes=[dma((3,))],
        )(*made)

    in_specs = (
        P("groups", "patch", None, None),
        P("groups", "patch", None, None),
        P(None, "groups", "patch", None, None),
        P("groups"),
        P(),
        P(),
        P(),
        P(),
        P(),
    )
    out_specs = (
        P("groups", "patch", None, None),
        P("groups", "patch", None, None),
        P(None, "groups", "patch", None, None),
    )
    return jax.shard_map(local, mesh=mesh, in_specs=in_specs, out_specs=out_specs, check_vma=False)
```

```python
import functools
import math

import jax
import jax.numpy as jnp
from jax import lax
from jax.experimental import pallas as pl
from jax.experimental.pallas import tpu as pltpu
from jax.sharding import PartitionSpec as P

HEAD_DIM = 64
PACK = 4
EPS = 1e-05
PUMPS = (1, 1, 1, 1, 0, 1, 1, 1)
BETWEEN = (3,)


def snake_width(mesh):
    try:
        axis = mesh.axis_names.index("patch")
        line = mesh.devices
        for other in range(line.ndim - 1, -1, -1):
            if other != axis:
                line = line.take(0, axis=other)
        rows = {tuple(d.coords)[1] for d in line.flat}
        return 2 if len(rows) == 2 and tuple(line.flat[2].coords)[1] != tuple(line.flat[0].coords)[1] else 1
    except Exception:
        return 1


def ring_pos(chip, chips, width):
    if width == 1:
        return chip
    long = chips // 2
    z, y = chip // 2, chip % 2
    return z * (1 - y) + (2 * long - 1 - z) * y


def ring_chip(pos, chips, width):
    if width == 1:
        return pos
    long = chips // 2
    y = pos // long
    z = pos * (1 - y) + (2 * long - 1 - pos) * y
    return z * 2 + y


def body(n, width, t_hbm, lat_hbm, stale_hbm, ssum_hbm, gain_hbm, conv_hbm, time_hbm, qkv_hbm, out_hbm,
         block_ref, states_ref, nsums_ref,
         t_ref, lat_ref, stale_ref, gain_ref, conv_w, time_w, qkv_w, out_w, halo, sums_all, sums_out, rx, keys, values,
         act, q_s, flip_w, max_s, den_s, mix_s, block_s, states_s,
         w_sem, small_sem, ring_send, ring_recv, core_send, core_recv, halo_send, halo_recv, sum_send, sum_recv, known):
    images, _, columns, channels = lat_ref.shape
    groups = ssum_hbm.shape[-1]
    f32, bf16 = jnp.float32, jnp.bfloat16
    tokens = images * columns
    chips, last = n // 2, n // 4
    count = float(n * columns * (channels // groups))
    me = lax.axis_index("patch")
    core = me % 2
    pos = ring_pos(me // 2, chips, width)
    ahead = ring_chip((pos + 1) % chips, chips, width) * 2
    behind = ring_chip((pos + chips - 1) % chips, chips, width) * 2
    target = ahead * (1 - core) + behind * core + core
    sibling = me + 1 - 2 * core
    source = ahead * core + behind * (1 - core) + core
    late = me >= n // 2
    MESH = pl.DeviceIdType.MESH

    barrier = pltpu.get_barrier_semaphore()

    def greet(semaphore, where):
        pl.semaphore_signal(semaphore, inc=1, device_id={"patch": where}, device_id_type=MESH)

    greet(barrier, source)
    greet(barrier, sibling)

    def load(src, dst, index):
        return pltpu.make_async_copy(src, dst, w_sem.at[index])

    conv_loads = [
        [load(conv_hbm.at[a, c], conv_w.at[a, :, pl.ds(c * channels, channels)], 3 * a + c) for c in range(3)]
        for a in range(3)
    ]
    time_load = load(time_hbm, time_w, 9)
    qkv_loads = [load(qkv_hbm.at[i], qkv_w.at[i], 10 + i) for i in range(3)]
    out_load = load(out_hbm, out_w, 13)
    small = [
        pltpu.make_async_copy(src, dst, small_sem.at[i])
        for i, (src, dst) in enumerate(
            ((stale_hbm, stale_ref), (ssum_hbm, sums_all.at[0]), (lat_hbm, lat_ref), (t_hbm, t_ref), (gain_hbm, gain_ref))
        )
    ]
    for copy in small:
        copy.start()
    def remote(src, dst, send, recv, where):
        return pltpu.make_async_remote_copy(src_ref=src, dst_ref=dst, send_sem=send, recv_sem=recv,
                                            device_id={"patch": where}, device_id_type=MESH)

    def sum_copy(d):
        return remote(sums_all.at[0], sums_all.at[d], sum_send.at[d], sum_recv.at[d], (me + d) % n)

    def halo_copy(slot):
        where = (me + 1) % n if slot == 0 else (me + n - 1) % n
        return remote(lat_ref, halo.at[slot], halo_send.at[slot], halo_recv.at[slot], where)

    def slot_of(step, direction, row, final):
        return 2 + 4 * (step - 1) + row + (0 if final else 2 * direction)

    def chunk(i, direction):
        return (direction if i < images else 1 - direction), i % images

    def ring_copy(step, i, first=False, final=False):
        row, image = chunk(i, core)
        if first:
            src = stale_ref.at[image, 0] if i < images else rx.at[image, 1]
        else:
            src = rx.at[image, slot_of(step - 1, core, row, False)]
        return remote(src, rx.at[image, slot_of(step, core, row, final)],
                      ring_send.at[step, i], ring_recv.at[step, i], target)

    def core_copy(step, i, final, direction=None):
        direction = core if direction is None else direction
        row, image = chunk(i, direction)
        ref = rx.at[image, slot_of(step, direction, row, final)]
        return remote(ref, ref, core_send.at[step, i], core_recv.at[step, i], sibling)

    def share_copies(step, direction=None):
        direction = core if direction is None else direction
        start = slot_of(step, direction, 0, False)
        begin = pl.multiple_of(start * columns, 2 * columns)
        refs = [keys.at[b, pl.ds(start, 2)] for b in range(images)]
        refs += [values.at[b, :, pl.ds(begin, 2 * columns)] for b in range(images)]
        return [
            remote(ref, ref, core_send.at[step, i], core_recv.at[step, i], sibling) for i, ref in enumerate(refs)
        ]

    def share(step):
        for copy in share_copies(step):
            copy.start()

    def own_core_copy(image):
        return remote(stale_ref.at[image, 0], rx.at[image, 1], core_send.at[0, image],
                      core_recv.at[0, image], sibling)

    for copy in small:
        copy.wait()
    time_load.start()
    qkv_loads[2].start()
    qkv_loads[1].start()
    for a in (1, 0, 2):
        for c in range(3):
            conv_loads[a][c].start()
    qkv_loads[0].start()
    out_load.start()
    pl.semaphore_wait(barrier, 2)

    greet(known.at[0], target)
    for image in range(images):
        own_core_copy(image).start()
    for image in range(images):
        ring_copy(1, image, first=True).start()

    @pl.when(core == 0)
    def _():
        halo_copy(0).start()

    @pl.when(core == 1)
    def _():
        halo_copy(1).start()

    def heard(spread):
        pl.semaphore_wait(known.at[spread], 1)
        if not isinstance(spread, int) or spread < last - 1:
            greet(known.at[spread + 1], target)

    def heard_first():
        @pl.loop(0, last - 2)
        def _(spread):
            heard(spread)

    pl.when(late)(heard_first)

    for image in range(images):
        own_core_copy(image).wait_recv()
        ring_copy(1, images + image, first=True).start()

    pl.when(jnp.logical_not(late))(heard_first)

    def event(step, i, kind):
        ring_copy(step, i, first=True, final=kind == 2).wait_recv()
        if kind == 0 or (kind == 1 and i < images):
            ring_copy(step + 1, i, final=kind == 1).start()
        if kind:
            core_copy(step, i, kind == 2).start()

    def count_of(kind):
        return images if kind == 2 else 2 * images

    def kind_of(step):
        return 2 if step == last else 1 if step == last - 1 else 0

    static = [s for s in range(1, last + 1) if last <= 4 or s <= 2]
    queue = [(s, i, kind_of(s)) for s in static for i in range(count_of(kind_of(s)))]

    def pump(amount=1):
        for _ in range(min(amount, len(queue))):
            event(*queue.pop(0))

    def drain(step):
        while queue and queue[0][0] <= step:
            pump()

    def forward(step, kind):
        for i in range(count_of(kind)):
            event(step, i, kind)

    @pl.when(me == 0)
    def _():
        halo[0] = jnp.zeros_like(lat_ref)

    @pl.when(me == n - 1)
    def _():
        halo[1] = jnp.zeros_like(lat_ref)

    across = (((1,), (1,)), ((), ()))

    def project_made(pieces):
        rows = jnp.concatenate([piece[2] for piece in pieces], axis=0)
        made = jnp.dot(rows, qkv_w[1], preferred_element_type=f32).astype(bf16)
        turned = lax.dot_general(flip_w[...], rows, across, preferred_element_type=f32).astype(bf16)
        span = 2 * columns
        for i, (image, start, _) in enumerate(pieces):
            at = slice(i * span, (i + 1) * span)
            begin = start * columns
            if not isinstance(begin, int):
                begin = pl.multiple_of(begin, span)
            keys[image, pl.ds(start, 2)] = made[at].reshape(2, columns, channels)
            values[image, :, pl.ds(begin, span)] = turned[:, at]

    def held(image, start):
        return image, start, rx[image, pl.ds(start, 2)].reshape(2 * columns, channels)

    def project(*steps):
        project_made([held(b, slot_of(step, core, 0, False)) for step in steps for b in range(images)])

    def arrived(step):
        for copy in share_copies(step, 1 - core):
            copy.wait_recv()

    def project_raw(step, final):
        for i in range(images if final else 2 * images):
            core_copy(step, i, final, direction=1 - core).wait_recv()
        first = slot_of(step, 0, 0, final)
        starts = [first] if final else [first, first + 2]
        project_made([held(b, start) for b in range(images) for start in starts])

    ch = lax.broadcasted_iota(jnp.int32, (channels, groups), 0)
    gr = lax.broadcasted_iota(jnp.int32, (channels, groups), 1) * (channels // groups)
    member = jnp.where((ch >= gr) & (ch < gr + channels // groups), 1.0, 0.0).astype(bf16)
    ch_t = lax.broadcasted_iota(jnp.int32, (groups, channels), 1)
    gr_t = lax.broadcasted_iota(jnp.int32, (groups, channels), 0) * (channels // groups)
    member_t = jnp.where((ch_t >= gr_t) & (ch_t < gr_t + channels // groups), 1.0, 0.0).astype(bf16)

    def exact(x, picks):
        rows = x.shape[0]
        hi = x.astype(bf16)
        rest = x - hi.astype(f32)
        mid = rest.astype(bf16)
        lo = (rest - mid.astype(f32)).astype(bf16)
        y = jnp.dot(jnp.concatenate([hi, mid, lo], axis=0), picks, preferred_element_type=f32)
        return y[2 * rows :] + y[rows : 2 * rows] + y[:rows]

    firsts = [queue.pop(0) for _ in range(3)]

    @pl.when(jnp.logical_not(late))
    def _():
        event(*firsts[0])

    heard(last - 2)

    @pl.when(jnp.logical_not(late))
    def _():
        event(*firsts[1])
        event(*firsts[2])

    heard(last - 1)
    greet(known.at[last], sibling)
    pl.semaphore_wait(known.at[last], 1)

    @pl.loop(1, n)
    def _(d):
        sum_copy(d).start()

    @pl.when((core == 1) & (me < n - 1))
    def _():
        halo_copy(0).start()

    @pl.when((core == 0) & (me > 0))
    def _():
        halo_copy(1).start()

    @pl.when(late)
    def _():
        for first in firsts:
            event(*first)

    freq_count = time_w.shape[0] // 2
    idx = lax.broadcasted_iota(jnp.int32, (8, 2 * freq_count), 1)
    low = idx < freq_count
    freqs = jnp.exp(-math.log(10000.0) * jnp.where(low, idx, idx - freq_count).astype(f32) / freq_count)
    angles = t_ref[...].astype(f32) * freqs
    emb = jnp.where(low, jnp.cos(angles), jnp.sin(angles))
    emb = emb / (1.0 + jnp.exp(-emb))
    time_load.wait()
    temb = exact(emb, time_w[...])[0:1]

    qkv_loads[2].wait()
    diagonal = lax.broadcasted_iota(jnp.int32, (channels, channels), 0) == lax.broadcasted_iota(
        jnp.int32, (channels, channels), 1
    )
    unit = jnp.where(diagonal, 1.0, 0.0).astype(bf16)
    flip_w[...] = lax.dot_general(unit, qkv_w[2], across, preferred_element_type=f32).astype(bf16)

    drain(1)
    qkv_loads[1].wait()
    project(1)
    pump(PUMPS[0])
    share(1)

    @pl.loop(1, n)
    def _(d):
        sum_copy(d).wait_recv()

    total = sums_all[0]
    total = lax.fori_loop(1, n, lambda d, acc: acc + sums_all[d], total)
    others = [total - sums_all[1], total - sums_all[0], total - sums_all[n - 1]]

    @pl.when(me > 0)
    def _():
        halo_copy(0).wait_recv()

    @pl.when(me < n - 1)
    def _():
        halo_copy(1).wait_recv()

    pump(PUMPS[1])

    def stacked(rows, size):
        pad = size - len(rows)
        if pad:
            rows = rows + [jnp.zeros((pad, rows[0].shape[1]), f32)]
        return jnp.concatenate(rows, axis=0)

    def statistics(blocks, norm, others_of):
        size = -(-len(blocks) // 8) * 8
        firsts = stacked([jnp.sum(x, axis=0, keepdims=True) for x in blocks], size)
        seconds = stacked([jnp.sum(x * x, axis=0, keepdims=True) for x in blocks], size)
        fresh = exact(jnp.concatenate([firsts, seconds], axis=0), member)
        fresh1, fresh2 = fresh[:size], fresh[size:]
        one = stacked([o[norm, b, 0, 0:1] for o, b in others_of], size)
        two = stacked([o[norm, b, 0, 1:2] for o, b in others_of], size)
        m = (one + fresh1) / count
        v = (two + fresh2) / count - m * m
        inv = lax.rsqrt(v + EPS)
        wide = exact(jnp.concatenate([m, inv], axis=0), member_t)
        return fresh1, fresh2, wide[:size], wide[size:]

    def widened(row, image):
        src = lat_ref[image, 0] if row == 1 else halo[0 if row == 0 else 1, image, 0]
        return src.astype(f32)

    pairs = [(r, b) for r in range(3) for b in range(images)]
    fresh1, fresh2, mean, inv = statistics([widened(r, b) for r, b in pairs], 0, [(others[r], b) for r, b in pairs])
    for b in range(images):
        i = images + b
        sums_out[0, b, 0, 0:1] = fresh1[i : i + 1]
        sums_out[0, b, 0, 1:2] = fresh2[i : i + 1]
    pump(PUMPS[2])
    inside = [jnp.where(me > 0, 1.0, 0.0).astype(f32), None, jnp.where(me < n - 1, 1.0, 0.0).astype(f32)]
    for i, (r, b) in enumerate(pairs):
        u = (widened(r, b) - mean[i : i + 1]) * inv[i : i + 1] * gain_ref[0:1, :]
        u = u / (1.0 + jnp.exp(-u))
        if inside[r] is not None:
            u = u * inside[r]
        act[r, pl.ds(b * columns, columns)] = u.astype(bf16)

    taps = None
    for a in (1, 0, 2):
        for c in range(3):
            conv_loads[a][c].wait()
        part = jnp.dot(act[a], conv_w[a], preferred_element_type=f32)
        taps = part if taps is None else taps + part
    taps = [taps[:, c * channels : (c + 1) * channels] for c in range(3)]

    place = lax.broadcasted_iota(jnp.int32, (tokens, channels), 0)
    first_col = place == 0
    last_col = place == columns - 1
    for b in range(1, images):
        first_col = first_col | (place == b * columns)
        last_col = last_col | (place == (b + 1) * columns - 1)
    conv = jnp.where(first_col, 0.0, pltpu.roll(taps[0], 1, 0)) + taps[1]
    conv = conv + jnp.where(last_col, 0.0, pltpu.roll(taps[2], tokens - 1, 0))
    pump(PUMPS[3])
    if last <= 4:
        for step in range(2, last - 1):
            drain(step)
            project(step)
            share(step)
    lat = jnp.concatenate([widened(1, b) for b in range(images)], axis=0)
    hidden = (lat + conv + temb).astype(bf16)
    wide_hidden = hidden.astype(f32)
    blocks = [wide_hidden[b * columns : (b + 1) * columns] for b in range(images)]
    fresh1, fresh2, mean, inv = statistics(blocks, 1, [(others[1], b) for b in range(images)])
    normed = []
    for b in range(images):
        sums_out[1, b, 0, 0:1] = fresh1[b : b + 1]
        sums_out[1, b, 0, 1:2] = fresh2[b : b + 1]
        s = ((blocks[b] - mean[b : b + 1]) * inv[b : b + 1] * gain_ref[1:2, :]).astype(bf16)
        states_s[b, 0] = s
        normed.append(s)
    states = jnp.concatenate(normed, axis=0)
    store_sums = pltpu.make_async_copy(sums_out.at[pl.ds(0, 2)], nsums_ref, small_sem.at[5])
    store_sums.start()
    store_states = pltpu.make_async_copy(states_s, states_ref, small_sem.at[6])
    store_states.start()
    pump(PUMPS[5])

    qkv_loads[0].wait()
    q_s[...] = jnp.dot(states, qkv_w[0], preferred_element_type=f32).astype(bf16)
    project_made([(b, 0, jnp.concatenate([normed[b], rx[b, 1]], axis=0)) for b in range(images)])
    pump(PUMPS[6])

    factor = math.log2(math.e) / math.sqrt(HEAD_DIM)

    pair = 2 * columns

    def sent():
        store_sums.wait()
        store_states.wait()

        @pl.loop(1, n)
        def _(d):
            sum_copy(d).wait_send()

        @pl.when(me < n - 1)
        def _():
            halo_copy(0).wait_send()

        @pl.when(me > 0)
        def _():
            halo_copy(1).wait_send()

        for image in range(images):
            own_core_copy(image).wait_send()
        for i in range(2 * images):
            ring_copy(1, i, first=True).wait_send()

            @pl.loop(2, last)
            def _(step):
                ring_copy(step, i).wait_send()

        @pl.loop(1, last - 1)
        def _(step):
            for copy in share_copies(step):
                copy.wait_send()

    def attend(start, size, begin, end, between=()):
        spans = [
            (b, c0, min(c0 + PACK * HEAD_DIM, channels))
            for b in range(images)
            for c0 in range(0, channels, PACK * HEAD_DIM)
        ]

        def score(b, c0, c1):
            heads = (c1 - c0) // HEAD_DIM
            qt = q_s[pl.ds(b * columns, columns), c0:c1]
            lane = lax.broadcasted_iota(jnp.int32, (columns, c1 - c0), 1)
            own = [(lane >= h * HEAD_DIM) & (lane < (h + 1) * HEAD_DIM) for h in range(heads)]
            qb = jnp.concatenate([jnp.where(own[h], qt, jnp.zeros_like(qt)) for h in range(heads)], axis=0)
            kk = keys[b, pl.ds(start, size), :, c0:c1].reshape(size * columns, c1 - c0)
            return lax.dot_general(kk, qb, across, preferred_element_type=f32)

        blocks_of = [[] for _ in range(images)]
        ahead_s = score(*spans[0])
        for pack, (b, c0, c1) in enumerate(spans):
            heads = (c1 - c0) // HEAD_DIM
            rows = heads * columns
            s = ahead_s
            if pack + 1 < len(spans):
                ahead_s = score(*spans[pack + 1])
            if pack in between:
                pump()
            vv = values[b, c0:c1, pl.ds(start * columns, size * columns)]
            top = jnp.max(s, axis=0, keepdims=True)
            if not begin:
                before = max_s[pack, :, pl.ds(0, rows)]
                top = jnp.maximum(top, before)
            e = jnp.exp2((s - top) * factor)
            den = jnp.sum(e, axis=0, keepdims=True)
            if not begin:
                scale = jnp.exp2((before - top) * factor)
                den = den + den_s[pack, :, pl.ds(0, rows)] * scale
            o = jnp.dot(vv, e.astype(bf16), preferred_element_type=f32)
            if not end:
                max_s[pack, :, pl.ds(0, rows)] = top
                den_s[pack, :, pl.ds(0, rows)] = den
            for h in range(heads):
                j = h // 2 * pair
                at = pl.ds(c0 + h * HEAD_DIM, HEAD_DIM)
                part = o[h * HEAD_DIM : (h + 1) * HEAD_DIM, j : j + pair]
                if not begin:
                    part = part + mix_s[b, at] * scale[:, j : j + pair]
                if not end:
                    mix_s[b, at] = part
                else:
                    part = part / den[:, j : j + pair]
                    blocks_of[b].append(part if h % 2 == b % 2 else pltpu.roll(part, columns, 1))
        if end:
            lane = lax.broadcasted_iota(jnp.int32, (HEAD_DIM, pair), 1)
            merged = [jnp.where(lane < columns, x, y) for x, y in zip(*blocks_of)]
            return jnp.concatenate(merged, axis=0).astype(bf16)

    if last > 4:
        drain(2)

        @pl.loop(3, last - 1)
        def _(step):
            forward(step, 0)
            project(step - 1)
            share(step - 1)

        project(last - 2)
        share(last - 2)

    @pl.loop(1, last - 1)
    def _(step):
        arrived(step)

    cut = slot_of(last - 1, 0, 0, False)
    if last <= 4:
        pump(PUMPS[7])
    attend(0, cut, True, False, BETWEEN)
    sent()
    if last <= 4:
        drain(last - 1)
    else:
        forward(last - 1, 1)
        forward(last, 2)
    if last <= 4:
        drain(last)
    project_raw(last - 1, False)
    project_raw(last, True)
    attended = attend(cut, n - cut, False, True)

    out_load.wait()
    result = wide_hidden + lax.dot_general(
        attended, out_w[...], (((0,), (0,)), ((), ())), preferred_element_type=f32
    )
    for b in range(images):
        block_s[b, 0] = result[b * columns : (b + 1) * columns].astype(bf16)
    store_block = pltpu.make_async_copy(block_s, block_ref, small_sem.at[7])
    store_block.start()
    for i in range(2 * images):
        core_copy(last - 1, i, False).wait_send()
    for i in range(images):
        ring_copy(last, i, final=True).wait_send()
        core_copy(last, i, True).wait_send()
    store_block.wait()


def settle(block_in, states_in, sums_in, block_ref, states_ref, sums_ref, sem):
    copies = [
        pltpu.make_async_copy(src, dst, sem.at[i])
        for i, (src, dst) in enumerate(((block_in, block_ref), (states_in, states_ref), (sums_in, sums_ref)))
    ]
    for copy in copies:
        copy.start()
    for copy in copies:
        copy.wait()


def solution(mesh):
    n = mesh.shape["patch"]
    width = snake_width(mesh)

    def local(latent, stale_states, stale_sums, timestep, norm_gain, conv_weight, time_weight, qkv_weight, out_weight):
        images, row_count, columns, channels = latent.shape
        assert row_count == 1 and n % 4 == 0 and n >= 8 and images == 2 and columns == HEAD_DIM
        vmem = pl.BlockSpec(memory_space=pltpu.VMEM)
        anywhere = pl.BlockSpec(memory_space=pl.ANY)
        bf16 = jnp.bfloat16
        dma = pltpu.SemaphoreType.DMA
        steps = n // 4 + 1
        packs = images * -(-channels // (PACK * HEAD_DIM))
        made = pl.pallas_call(
            functools.partial(body, n, width),
            out_shape=(
                jax.ShapeDtypeStruct(latent.shape, bf16),
                jax.ShapeDtypeStruct(latent.shape, bf16),
                jax.ShapeDtypeStruct(stale_sums.shape, jnp.float32),
            ),
            in_specs=[pl.BlockSpec(memory_space=pltpu.HBM)] * 9,
            out_specs=(pl.BlockSpec(memory_space=pltpu.HBM),) * 3,
            scratch_shapes=[
                pltpu.VMEM((1, 1), jnp.int32),
                pltpu.VMEM(latent.shape, bf16),
                pltpu.VMEM(latent.shape, bf16),
                pltpu.VMEM(norm_gain.shape, jnp.float32),
                pltpu.VMEM((3, channels, 3 * channels), bf16),
                pltpu.VMEM(time_weight.shape, bf16),
                pltpu.VMEM(qkv_weight.shape, bf16),
                pltpu.VMEM(out_weight.shape, bf16),
                pltpu.VMEM((2,) + latent.shape, bf16),
                pltpu.VMEM((n + 1,) + stale_sums.shape, jnp.float32),
                pltpu.VMEM((3,) + stale_sums.shape[1:], jnp.float32),
                pltpu.VMEM((images, n, columns, channels), bf16),
                pltpu.VMEM((images, n, columns, channels), bf16),
                pltpu.VMEM((images, channels, n * columns), bf16),
                pltpu.VMEM((3, images * columns, channels), bf16),
                pltpu.VMEM((images * columns, channels), bf16),
                pltpu.VMEM((channels, channels), bf16),
                pltpu.VMEM((packs, 1, PACK * columns), jnp.float32),
                pltpu.VMEM((packs, 1, PACK * columns), jnp.float32),
                pltpu.VMEM((images, channels, 2 * columns), jnp.float32),
                pltpu.VMEM(latent.shape, bf16),
                pltpu.VMEM(latent.shape, bf16),
                dma((14,)),
                dma((8,)),
                dma((steps, 2 * images)),
                dma((steps, 2 * images)),
                dma((steps, 2 * images)),
                dma((steps, 2 * images)),
                dma((2,)),
                dma((2,)),
                dma((n,)),
                dma((n,)),
                pltpu.SemaphoreType.REGULAR((n // 4 + 1,)),
            ],
            compiler_params=pltpu.CompilerParams(
                collective_id=0, has_side_effects=True, vmem_limit_bytes=60 * 1024 * 1024
            ),
        )(timestep.reshape(1, 1), latent, stale_states, stale_sums, norm_gain, conv_weight, time_weight, qkv_weight, out_weight)
        return pl.pallas_call(
            settle,
            out_shape=tuple(jax.ShapeDtypeStruct(x.shape, x.dtype) for x in made),
            in_specs=[vmem] * 3,
            out_specs=(anywhere,) * 3,
            scratch_shapes=[dma((3,))],
        )(*made)

    in_specs = (
        P("groups", "patch", None, None),
        P("groups", "patch", None, None),
        P(None, "groups", "patch", None, None),
        P("groups"),
        P(),
        P(),
        P(),
        P(),
        P(),
    )
    out_specs = (
        P("groups", "patch", None, None),
        P("groups", "patch", None, None),
        P(None, "groups", "patch", None, None),
    )
    return jax.shard_map(local, mesh=mesh, in_specs=in_specs, out_specs=out_specs, check_vma=False)
```

```python
import functools
import math

import jax
import jax.numpy as jnp
from jax import lax
from jax.experimental import pallas as pl
from jax.experimental.pallas import tpu as pltpu
from jax.sharding import PartitionSpec as P

HEAD_DIM = 64
PACK = 4
EPS = 1e-05
PUMPS = (2, 1, 1, 1, 0, 1, 1, 1)
BETWEEN = (3,)


def snake_width(mesh):
    try:
        axis = mesh.axis_names.index("patch")
        line = mesh.devices
        for other in range(line.ndim - 1, -1, -1):
            if other != axis:
                line = line.take(0, axis=other)
        rows = {tuple(d.coords)[1] for d in line.flat}
        return 2 if len(rows) == 2 and tuple(line.flat[2].coords)[1] != tuple(line.flat[0].coords)[1] else 1
    except Exception:
        return 1


def ring_pos(chip, chips, width):
    if width == 1:
        return chip
    long = chips // 2
    z, y = chip // 2, chip % 2
    return z * (1 - y) + (2 * long - 1 - z) * y


def ring_chip(pos, chips, width):
    if width == 1:
        return pos
    long = chips // 2
    y = pos // long
    z = pos * (1 - y) + (2 * long - 1 - pos) * y
    return z * 2 + y


def body(n, width, t_hbm, lat_hbm, stale_hbm, ssum_hbm, gain_hbm, conv_hbm, time_hbm, qkv_hbm, out_hbm,
         block_ref, states_ref, nsums_ref,
         t_ref, lat_ref, stale_ref, gain_ref, conv_w, time_w, qkv_w, out_w, halo, sums_all, sums_out, rx, keys, values,
         act, q_s, flip_w, max_s, den_s, mix_s, block_s, states_s,
         w_sem, small_sem, ring_send, ring_recv, core_send, core_recv, halo_send, halo_recv, sum_send, sum_recv, known):
    images, _, columns, channels = lat_ref.shape
    groups = ssum_hbm.shape[-1]
    f32, bf16 = jnp.float32, jnp.bfloat16
    tokens = images * columns
    chips, last = n // 2, n // 4
    count = float(n * columns * (channels // groups))
    me = lax.axis_index("patch")
    core = me % 2
    pos = ring_pos(me // 2, chips, width)
    ahead = ring_chip((pos + 1) % chips, chips, width) * 2
    behind = ring_chip((pos + chips - 1) % chips, chips, width) * 2
    target = ahead * (1 - core) + behind * core + core
    sibling = me + 1 - 2 * core
    source = ahead * core + behind * (1 - core) + core
    late = me >= n // 2
    MESH = pl.DeviceIdType.MESH

    barrier = pltpu.get_barrier_semaphore()

    def greet(semaphore, where):
        pl.semaphore_signal(semaphore, inc=1, device_id={"patch": where}, device_id_type=MESH)

    greet(barrier, source)
    greet(barrier, sibling)

    def load(src, dst, index):
        return pltpu.make_async_copy(src, dst, w_sem.at[index])

    conv_loads = [
        [load(conv_hbm.at[a, c], conv_w.at[a, :, pl.ds(c * channels, channels)], 3 * a + c) for c in range(3)]
        for a in range(3)
    ]
    time_load = load(time_hbm, time_w, 9)
    qkv_loads = [load(qkv_hbm.at[i], qkv_w.at[i], 10 + i) for i in range(3)]
    out_load = load(out_hbm, out_w, 13)
    small = [
        pltpu.make_async_copy(src, dst, small_sem.at[i])
        for i, (src, dst) in enumerate(
            ((stale_hbm, stale_ref), (ssum_hbm, sums_all.at[0]), (lat_hbm, lat_ref), (t_hbm, t_ref), (gain_hbm, gain_ref))
        )
    ]
    for copy in small:
        copy.start()
    def remote(src, dst, send, recv, where):
        return pltpu.make_async_remote_copy(src_ref=src, dst_ref=dst, send_sem=send, recv_sem=recv,
                                            device_id={"patch": where}, device_id_type=MESH)

    def sum_copy(d):
        return remote(sums_all.at[0], sums_all.at[d], sum_send.at[d], sum_recv.at[d], (me + d) % n)

    def halo_copy(slot):
        where = (me + 1) % n if slot == 0 else (me + n - 1) % n
        return remote(lat_ref, halo.at[slot], halo_send.at[slot], halo_recv.at[slot], where)

    def slot_of(step, direction, row, final):
        return 2 + 4 * (step - 1) + row + (0 if final else 2 * direction)

    def chunk(i, direction):
        return (direction if i < images else 1 - direction), i % images

    def ring_copy(step, i, first=False, final=False):
        row, image = chunk(i, core)
        if first:
            src = stale_ref.at[image, 0] if i < images else rx.at[image, 1]
        else:
            src = rx.at[image, slot_of(step - 1, core, row, False)]
        return remote(src, rx.at[image, slot_of(step, core, row, final)],
                      ring_send.at[step, i], ring_recv.at[step, i], target)

    def core_copy(step, i, final, direction=None):
        direction = core if direction is None else direction
        row, image = chunk(i, direction)
        ref = rx.at[image, slot_of(step, direction, row, final)]
        return remote(ref, ref, core_send.at[step, i], core_recv.at[step, i], sibling)

    def share_copies(step, direction=None):
        direction = core if direction is None else direction
        start = slot_of(step, direction, 0, False)
        begin = pl.multiple_of(start * columns, 2 * columns)
        refs = [keys.at[b, pl.ds(start, 2)] for b in range(images)]
        refs += [values.at[b, :, pl.ds(begin, 2 * columns)] for b in range(images)]
        return [
            remote(ref, ref, core_send.at[step, i], core_recv.at[step, i], sibling) for i, ref in enumerate(refs)
        ]

    def share(step):
        for copy in share_copies(step):
            copy.start()

    def own_core_copy(image):
        return remote(stale_ref.at[image, 0], rx.at[image, 1], core_send.at[0, image],
                      core_recv.at[0, image], sibling)

    for copy in small:
        copy.wait()
    time_load.start()
    qkv_loads[2].start()
    qkv_loads[1].start()
    for a in (1, 0, 2):
        for c in range(3):
            conv_loads[a][c].start()
    qkv_loads[0].start()
    out_load.start()
    pl.semaphore_wait(barrier, 2)

    greet(known.at[0], target)
    for image in range(images):
        own_core_copy(image).start()
    for image in range(images):
        ring_copy(1, image, first=True).start()

    @pl.when(core == 0)
    def _():
        halo_copy(0).start()

    @pl.when(core == 1)
    def _():
        halo_copy(1).start()

    def heard(spread):
        pl.semaphore_wait(known.at[spread], 1)
        if not isinstance(spread, int) or spread < last - 1:
            greet(known.at[spread + 1], target)

    def heard_first():
        @pl.loop(0, last - 2)
        def _(spread):
            heard(spread)

    pl.when(late)(heard_first)

    for image in range(images):
        own_core_copy(image).wait_recv()
        ring_copy(1, images + image, first=True).start()

    pl.when(jnp.logical_not(late))(heard_first)

    def event(step, i, kind):
        ring_copy(step, i, first=True, final=kind == 2).wait_recv()
        if kind == 0 or (kind == 1 and i < images):
            ring_copy(step + 1, i, final=kind == 1).start()
        if kind:
            core_copy(step, i, kind == 2).start()

    def count_of(kind):
        return images if kind == 2 else 2 * images

    def kind_of(step):
        return 2 if step == last else 1 if step == last - 1 else 0

    static = [s for s in range(1, last + 1) if last <= 4 or s <= 2]
    queue = [(s, i, kind_of(s)) for s in static for i in range(count_of(kind_of(s)))]

    def pump(amount=1):
        for _ in range(min(amount, len(queue))):
            event(*queue.pop(0))

    def drain(step):
        while queue and queue[0][0] <= step:
            pump()

    def forward(step, kind):
        for i in range(count_of(kind)):
            event(step, i, kind)

    @pl.when(me == 0)
    def _():
        halo[0] = jnp.zeros_like(lat_ref)

    @pl.when(me == n - 1)
    def _():
        halo[1] = jnp.zeros_like(lat_ref)

    across = (((1,), (1,)), ((), ()))

    def project_made(pieces):
        rows = jnp.concatenate([piece[2] for piece in pieces], axis=0)
        made = jnp.dot(rows, qkv_w[1], preferred_element_type=f32).astype(bf16)
        turned = lax.dot_general(flip_w[...], rows, across, preferred_element_type=f32).astype(bf16)
        span = 2 * columns
        for i, (image, start, _) in enumerate(pieces):
            at = slice(i * span, (i + 1) * span)
            begin = start * columns
            if not isinstance(begin, int):
                begin = pl.multiple_of(begin, span)
            keys[image, pl.ds(start, 2)] = made[at].reshape(2, columns, channels)
            values[image, :, pl.ds(begin, span)] = turned[:, at]

    def held(image, start):
        return image, start, rx[image, pl.ds(start, 2)].reshape(2 * columns, channels)

    def project(*steps):
        project_made([held(b, slot_of(step, core, 0, False)) for step in steps for b in range(images)])

    def arrived(step):
        for copy in share_copies(step, 1 - core):
            copy.wait_recv()

    def project_raw(step, final):
        for i in range(images if final else 2 * images):
            core_copy(step, i, final, direction=1 - core).wait_recv()
        first = slot_of(step, 0, 0, final)
        starts = [first] if final else [first, first + 2]
        project_made([held(b, start) for b in range(images) for start in starts])

    ch = lax.broadcasted_iota(jnp.int32, (channels, groups), 0)
    gr = lax.broadcasted_iota(jnp.int32, (channels, groups), 1) * (channels // groups)
    member = jnp.where((ch >= gr) & (ch < gr + channels // groups), 1.0, 0.0).astype(bf16)
    ch_t = lax.broadcasted_iota(jnp.int32, (groups, channels), 1)
    gr_t = lax.broadcasted_iota(jnp.int32, (groups, channels), 0) * (channels // groups)
    member_t = jnp.where((ch_t >= gr_t) & (ch_t < gr_t + channels // groups), 1.0, 0.0).astype(bf16)

    def exact(x, picks):
        rows = x.shape[0]
        hi = x.astype(bf16)
        rest = x - hi.astype(f32)
        mid = rest.astype(bf16)
        lo = (rest - mid.astype(f32)).astype(bf16)
        y = jnp.dot(jnp.concatenate([hi, mid, lo], axis=0), picks, preferred_element_type=f32)
        return y[2 * rows :] + y[rows : 2 * rows] + y[:rows]

    firsts = [queue.pop(0) for _ in range(3)]

    @pl.when(jnp.logical_not(late))
    def _():
        event(*firsts[0])

    heard(last - 2)

    @pl.when(jnp.logical_not(late))
    def _():
        event(*firsts[1])
        event(*firsts[2])

    heard(last - 1)
    greet(known.at[last], sibling)
    pl.semaphore_wait(known.at[last], 1)

    @pl.loop(1, n)
    def _(d):
        sum_copy(d).start()

    @pl.when((core == 1) & (me < n - 1))
    def _():
        halo_copy(0).start()

    @pl.when((core == 0) & (me > 0))
    def _():
        halo_copy(1).start()

    @pl.when(late)
    def _():
        for first in firsts:
            event(*first)

    freq_count = time_w.shape[0] // 2
    idx = lax.broadcasted_iota(jnp.int32, (8, 2 * freq_count), 1)
    low = idx < freq_count
    freqs = jnp.exp(-math.log(10000.0) * jnp.where(low, idx, idx - freq_count).astype(f32) / freq_count)
    angles = t_ref[...].astype(f32) * freqs
    emb = jnp.where(low, jnp.cos(angles), jnp.sin(angles))
    emb = emb / (1.0 + jnp.exp(-emb))
    time_load.wait()
    temb = exact(emb, time_w[...])[0:1]

    qkv_loads[2].wait()
    diagonal = lax.broadcasted_iota(jnp.int32, (channels, channels), 0) == lax.broadcasted_iota(
        jnp.int32, (channels, channels), 1
    )
    unit = jnp.where(diagonal, 1.0, 0.0).astype(bf16)
    flip_w[...] = lax.dot_general(unit, qkv_w[2], across, preferred_element_type=f32).astype(bf16)

    drain(1)
    qkv_loads[1].wait()
    project(1)
    pump(PUMPS[0])
    share(1)

    @pl.loop(1, n)
    def _(d):
        sum_copy(d).wait_recv()

    total = sums_all[0]
    total = lax.fori_loop(1, n, lambda d, acc: acc + sums_all[d], total)
    others = [total - sums_all[1], total - sums_all[0], total - sums_all[n - 1]]

    @pl.when(me > 0)
    def _():
        halo_copy(0).wait_recv()

    @pl.when(me < n - 1)
    def _():
        halo_copy(1).wait_recv()

    pump(PUMPS[1])

    def stacked(rows, size):
        pad = size - len(rows)
        if pad:
            rows = rows + [jnp.zeros((pad, rows[0].shape[1]), f32)]
        return jnp.concatenate(rows, axis=0)

    def statistics(blocks, norm, others_of):
        size = -(-len(blocks) // 8) * 8
        firsts = stacked([jnp.sum(x, axis=0, keepdims=True) for x in blocks], size)
        seconds = stacked([jnp.sum(x * x, axis=0, keepdims=True) for x in blocks], size)
        fresh = exact(jnp.concatenate([firsts, seconds], axis=0), member)
        fresh1, fresh2 = fresh[:size], fresh[size:]
        one = stacked([o[norm, b, 0, 0:1] for o, b in others_of], size)
        two = stacked([o[norm, b, 0, 1:2] for o, b in others_of], size)
        m = (one + fresh1) / count
        v = (two + fresh2) / count - m * m
        inv = lax.rsqrt(v + EPS)
        wide = exact(jnp.concatenate([m, inv], axis=0), member_t)
        return fresh1, fresh2, wide[:size], wide[size:]

    def widened(row, image):
        src = lat_ref[image, 0] if row == 1 else halo[0 if row == 0 else 1, image, 0]
        return src.astype(f32)

    pairs = [(r, b) for r in range(3) for b in range(images)]
    fresh1, fresh2, mean, inv = statistics([widened(r, b) for r, b in pairs], 0, [(others[r], b) for r, b in pairs])
    for b in range(images):
        i = images + b
        sums_out[0, b, 0, 0:1] = fresh1[i : i + 1]
        sums_out[0, b, 0, 1:2] = fresh2[i : i + 1]
    pump(PUMPS[2])
    inside = [jnp.where(me > 0, 1.0, 0.0).astype(f32), None, jnp.where(me < n - 1, 1.0, 0.0).astype(f32)]
    for i, (r, b) in enumerate(pairs):
        u = (widened(r, b) - mean[i : i + 1]) * inv[i : i + 1] * gain_ref[0:1, :]
        u = u / (1.0 + jnp.exp(-u))
        if inside[r] is not None:
            u = u * inside[r]
        act[r, pl.ds(b * columns, columns)] = u.astype(bf16)

    taps = None
    for a in (1, 0, 2):
        for c in range(3):
            conv_loads[a][c].wait()
        part = jnp.dot(act[a], conv_w[a], preferred_element_type=f32)
        taps = part if taps is None else taps + part
    taps = [taps[:, c * channels : (c + 1) * channels] for c in range(3)]

    place = lax.broadcasted_iota(jnp.int32, (tokens, channels), 0)
    first_col = place == 0
    last_col = place == columns - 1
    for b in range(1, images):
        first_col = first_col | (place == b * columns)
        last_col = last_col | (place == (b + 1) * columns - 1)
    conv = jnp.where(first_col, 0.0, pltpu.roll(taps[0], 1, 0)) + taps[1]
    conv = conv + jnp.where(last_col, 0.0, pltpu.roll(taps[2], tokens - 1, 0))
    pump(PUMPS[3])
    if last <= 4:
        for step in range(2, last - 1):
            drain(step)
            project(step)
            share(step)
    lat = jnp.concatenate([widened(1, b) for b in range(images)], axis=0)
    hidden = (lat + conv + temb).astype(bf16)
    wide_hidden = hidden.astype(f32)
    blocks = [wide_hidden[b * columns : (b + 1) * columns] for b in range(images)]
    fresh1, fresh2, mean, inv = statistics(blocks, 1, [(others[1], b) for b in range(images)])
    normed = []
    for b in range(images):
        sums_out[1, b, 0, 0:1] = fresh1[b : b + 1]
        sums_out[1, b, 0, 1:2] = fresh2[b : b + 1]
        s = ((blocks[b] - mean[b : b + 1]) * inv[b : b + 1] * gain_ref[1:2, :]).astype(bf16)
        states_s[b, 0] = s
        normed.append(s)
    states = jnp.concatenate(normed, axis=0)
    store_sums = pltpu.make_async_copy(sums_out.at[pl.ds(0, 2)], nsums_ref, small_sem.at[5])
    store_sums.start()
    store_states = pltpu.make_async_copy(states_s, states_ref, small_sem.at[6])
    store_states.start()
    pump(PUMPS[5])

    qkv_loads[0].wait()
    q_s[...] = jnp.dot(states, qkv_w[0], preferred_element_type=f32).astype(bf16)
    project_made([(b, 0, jnp.concatenate([normed[b], rx[b, 1]], axis=0)) for b in range(images)])
    pump(PUMPS[6])

    factor = math.log2(math.e) / math.sqrt(HEAD_DIM)

    pair = 2 * columns

    def sent():
        store_sums.wait()
        store_states.wait()

        @pl.loop(1, n)
        def _(d):
            sum_copy(d).wait_send()

        @pl.when(me < n - 1)
        def _():
            halo_copy(0).wait_send()

        @pl.when(me > 0)
        def _():
            halo_copy(1).wait_send()

        for image in range(images):
            own_core_copy(image).wait_send()
        for i in range(2 * images):
            ring_copy(1, i, first=True).wait_send()

            @pl.loop(2, last)
            def _(step):
                ring_copy(step, i).wait_send()

        @pl.loop(1, last - 1)
        def _(step):
            for copy in share_copies(step):
                copy.wait_send()

    def attend(start, size, begin, end, between=()):
        spans = [
            (b, c0, min(c0 + PACK * HEAD_DIM, channels))
            for b in range(images)
            for c0 in range(0, channels, PACK * HEAD_DIM)
        ]

        def score(b, c0, c1):
            heads = (c1 - c0) // HEAD_DIM
            qt = q_s[pl.ds(b * columns, columns), c0:c1]
            lane = lax.broadcasted_iota(jnp.int32, (columns, c1 - c0), 1)
            own = [(lane >= h * HEAD_DIM) & (lane < (h + 1) * HEAD_DIM) for h in range(heads)]
            qb = jnp.concatenate([jnp.where(own[h], qt, jnp.zeros_like(qt)) for h in range(heads)], axis=0)
            kk = keys[b, pl.ds(start, size), :, c0:c1].reshape(size * columns, c1 - c0)
            return lax.dot_general(kk, qb, across, preferred_element_type=f32)

        blocks_of = [[] for _ in range(images)]
        ahead_s = score(*spans[0])
        for pack, (b, c0, c1) in enumerate(spans):
            heads = (c1 - c0) // HEAD_DIM
            rows = heads * columns
            s = ahead_s
            if pack + 1 < len(spans):
                ahead_s = score(*spans[pack + 1])
            if pack in between:
                pump()
            vv = values[b, c0:c1, pl.ds(start * columns, size * columns)]
            top = jnp.max(s, axis=0, keepdims=True)
            if not begin:
                before = max_s[pack, :, pl.ds(0, rows)]
                top = jnp.maximum(top, before)
            e = jnp.exp2((s - top) * factor)
            den = jnp.sum(e, axis=0, keepdims=True)
            if not begin:
                scale = jnp.exp2((before - top) * factor)
                den = den + den_s[pack, :, pl.ds(0, rows)] * scale
            o = jnp.dot(vv, e.astype(bf16), preferred_element_type=f32)
            if not end:
                max_s[pack, :, pl.ds(0, rows)] = top
                den_s[pack, :, pl.ds(0, rows)] = den
            for h in range(heads):
                j = h // 2 * pair
                at = pl.ds(c0 + h * HEAD_DIM, HEAD_DIM)
                part = o[h * HEAD_DIM : (h + 1) * HEAD_DIM, j : j + pair]
                if not begin:
                    part = part + mix_s[b, at] * scale[:, j : j + pair]
                if not end:
                    mix_s[b, at] = part
                else:
                    part = part / den[:, j : j + pair]
                    blocks_of[b].append(part if h % 2 == b % 2 else pltpu.roll(part, columns, 1))
        if end:
            lane = lax.broadcasted_iota(jnp.int32, (HEAD_DIM, pair), 1)
            merged = [jnp.where(lane < columns, x, y) for x, y in zip(*blocks_of)]
            return jnp.concatenate(merged, axis=0).astype(bf16)

    if last > 4:
        drain(2)

        @pl.loop(3, last - 1)
        def _(step):
            forward(step, 0)
            project(step - 1)
            share(step - 1)

        project(last - 2)
        share(last - 2)

    @pl.loop(1, last - 1)
    def _(step):
        arrived(step)

    cut = slot_of(last - 1, 0, 0, False)
    if last <= 4:
        pump(PUMPS[7])
    attend(0, cut, True, False, BETWEEN)
    sent()
    if last <= 4:
        drain(last - 1)
    else:
        forward(last - 1, 1)
        forward(last, 2)
    if last <= 4:
        drain(last)
    project_raw(last - 1, False)
    project_raw(last, True)
    attended = attend(cut, n - cut, False, True)

    out_load.wait()
    result = wide_hidden + lax.dot_general(
        attended, out_w[...], (((0,), (0,)), ((), ())), preferred_element_type=f32
    )
    for b in range(images):
        block_s[b, 0] = result[b * columns : (b + 1) * columns].astype(bf16)
    store_block = pltpu.make_async_copy(block_s, block_ref, small_sem.at[7])
    store_block.start()
    for i in range(2 * images):
        core_copy(last - 1, i, False).wait_send()
    for i in range(images):
        ring_copy(last, i, final=True).wait_send()
        core_copy(last, i, True).wait_send()
    store_block.wait()


def settle(block_in, states_in, sums_in, block_ref, states_ref, sums_ref, sem):
    copies = [
        pltpu.make_async_copy(src, dst, sem.at[i])
        for i, (src, dst) in enumerate(((block_in, block_ref), (states_in, states_ref), (sums_in, sums_ref)))
    ]
    for copy in copies:
        copy.start()
    for copy in copies:
        copy.wait()


def solution(mesh):
    n = mesh.shape["patch"]
    width = snake_width(mesh)

    def local(latent, stale_states, stale_sums, timestep, norm_gain, conv_weight, time_weight, qkv_weight, out_weight):
        images, row_count, columns, channels = latent.shape
        assert row_count == 1 and n % 4 == 0 and n >= 8 and images == 2 and columns == HEAD_DIM
        vmem = pl.BlockSpec(memory_space=pltpu.VMEM)
        anywhere = pl.BlockSpec(memory_space=pl.ANY)
        bf16 = jnp.bfloat16
        dma = pltpu.SemaphoreType.DMA
        steps = n // 4 + 1
        packs = images * -(-channels // (PACK * HEAD_DIM))
        made = pl.pallas_call(
            functools.partial(body, n, width),
            out_shape=(
                jax.ShapeDtypeStruct(latent.shape, bf16),
                jax.ShapeDtypeStruct(latent.shape, bf16),
                jax.ShapeDtypeStruct(stale_sums.shape, jnp.float32),
            ),
            in_specs=[pl.BlockSpec(memory_space=pltpu.HBM)] * 9,
            out_specs=(pl.BlockSpec(memory_space=pltpu.HBM),) * 3,
            scratch_shapes=[
                pltpu.VMEM((1, 1), jnp.int32),
                pltpu.VMEM(latent.shape, bf16),
                pltpu.VMEM(latent.shape, bf16),
                pltpu.VMEM(norm_gain.shape, jnp.float32),
                pltpu.VMEM((3, channels, 3 * channels), bf16),
                pltpu.VMEM(time_weight.shape, bf16),
                pltpu.VMEM(qkv_weight.shape, bf16),
                pltpu.VMEM(out_weight.shape, bf16),
                pltpu.VMEM((2,) + latent.shape, bf16),
                pltpu.VMEM((n + 1,) + stale_sums.shape, jnp.float32),
                pltpu.VMEM((3,) + stale_sums.shape[1:], jnp.float32),
                pltpu.VMEM((images, n, columns, channels), bf16),
                pltpu.VMEM((images, n, columns, channels), bf16),
                pltpu.VMEM((images, channels, n * columns), bf16),
                pltpu.VMEM((3, images * columns, channels), bf16),
                pltpu.VMEM((images * columns, channels), bf16),
                pltpu.VMEM((channels, channels), bf16),
                pltpu.VMEM((packs, 1, PACK * columns), jnp.float32),
                pltpu.VMEM((packs, 1, PACK * columns), jnp.float32),
                pltpu.VMEM((images, channels, 2 * columns), jnp.float32),
                pltpu.VMEM(latent.shape, bf16),
                pltpu.VMEM(latent.shape, bf16),
                dma((14,)),
                dma((8,)),
                dma((steps, 2 * images)),
                dma((steps, 2 * images)),
                dma((steps, 2 * images)),
                dma((steps, 2 * images)),
                dma((2,)),
                dma((2,)),
                dma((n,)),
                dma((n,)),
                pltpu.SemaphoreType.REGULAR((n // 4 + 1,)),
            ],
            compiler_params=pltpu.CompilerParams(
                collective_id=0, has_side_effects=True, vmem_limit_bytes=60 * 1024 * 1024
            ),
        )(timestep.reshape(1, 1), latent, stale_states, stale_sums, norm_gain, conv_weight, time_weight, qkv_weight, out_weight)
        return pl.pallas_call(
            settle,
            out_shape=tuple(jax.ShapeDtypeStruct(x.shape, x.dtype) for x in made),
            in_specs=[vmem] * 3,
            out_specs=(anywhere,) * 3,
            scratch_shapes=[dma((3,))],
        )(*made)

    in_specs = (
        P("groups", "patch", None, None),
        P("groups", "patch", None, None),
        P(None, "groups", "patch", None, None),
        P("groups"),
        P(),
        P(),
        P(),
        P(),
        P(),
    )
    out_specs = (
        P("groups", "patch", None, None),
        P("groups", "patch", None, None),
        P(None, "groups", "patch", None, None),
    )
    return jax.shard_map(local, mesh=mesh, in_specs=in_specs, out_specs=out_specs, check_vma=False)
```
